256 devices in a mesh: tm: 16 (over z, y_hi), obs: 16 (over x, y_lo, core).
Axes of the slice: x: 4, y: 4 (y_hi: 2, y_lo: 2; y = y_hi * 2 + y_lo), z: 8, core: 2. Of those that a mesh axis runs over, the one named last changes fastest.
Arguments:
- trajectory: bfloat16 [16, 256, 256, 128], P('tm', 'obs'), may hold values from -6 to 6
- weights: bfloat16 [8192, 128, 256], P(('tm', 'obs')), may hold values from -0.375 to 0.375
- observed: bfloat16 [8192, 128, 128], P(('tm', 'obs')), may hold values from -9 to 9
- window: int32 [8192, 1], P(('tm', 'obs')), may hold values from 0 to 15; in each aligned block of 32 rows (0 to 31, 32 to 63, ...) at most 4 rows name the same one
- block: int32 [8192], P(('tm', 'obs')), may hold values from 0 to 15
- counts: int32 [8192], P(('tm', 'obs')), may hold values from 32 to 128, as said below
- flags: int32 [8192, 128], P(('tm', 'obs')), may hold values 0 or 1
- inv_error: float32 [128], replicated, may hold values from 0.5 to 2
Outputs:
- departures: bfloat16 [8192, 128, 128], P(('tm', 'obs'))
- window_bias: float32 [16, 128], P('tm')
- window_chi: float32 [16, 128], P('tm')
The draws below stay inside these ranges and needn't reach their ends.
Inputs may be any that keep to these rules, and one draw needn't show every extreme that they name: Among the 32 groups of one device, no sub-window is named by more than 4. `counts`: among the 32 groups of one device, one has all 128 slots live.
All inputs are finite; a program needn't handle non-finite values. No bound on the sum of `flags` on one device may be relied on, other than what follows from the above.
Results may differ from the reference program's by a relative error of at most 0.001.
Values may be sent and summed in bfloat16 or wider, within the bound.
A program may use at most 64 MiB of HBM per device.

```python
import math
import jax
import jax.numpy as jnp
import numpy as np
from jax import lax

LEV = 128
G = 256
BL = 16
CAPB = 128
NGRP = 32
GCAP = 4
NT = 16
NB = 256
NGRP_ALL = 8192
N_TM = 16
N_OBS = 16


def draw_counts(key, part):
    devices = N_TM * N_OBS
    first_key = jax.random.fold_in(key, 11)
    second_key = jax.random.fold_in(key, 23)
    values = jax.random.randint(first_key, (devices, NGRP), CAPB // 4, CAPB + 1)
    full_at = jax.random.randint(second_key, (devices,), 0, NGRP)
    column = jnp.arange(NGRP, dtype=jnp.int32)[None, :]
    values = jnp.where(column == full_at[:, None], CAPB, values)
    return values.reshape(devices * NGRP).astype(jnp.int32)


def place_ends(array, rng, least, high):
    place = [jax.random.randint(jax.random.fold_in(rng, axis), (), 0, length) for axis, length in enumerate(array.shape)]
    widest = array.shape.index(max(array.shape))
    neighbour = place[:widest] + [(place[widest] + 1) % array.shape[widest]] + place[widest + 1:]
    return array.at[tuple(place)].set(least).at[tuple(neighbour)].set(high)


def block_scale(own_key, shape, pieces, low, largest):
    loudness, own = 1.0, jax.random.fold_in(own_key, 6)
    for position, shards_of in pieces:
        steps = jnp.exp(jax.random.uniform(jax.random.fold_in(own, position), (shards_of,), jnp.float32, low / len(pieces), largest / len(pieces)))
        loudness = loudness * jnp.repeat(steps, shape[position] // shards_of).reshape([-1 if axis == position else 1 for axis in range(len(shape))])
    return loudness


def shared_out(stream_key, own, number, rows, number_of, top, bound, lean):
    ranking = jax.random.permutation(stream_key, number_of)
    packed, usual = load_shares(number_of, rows * top, bound, lean, True), load_shares(number_of, rows * top, bound, lean, False)
    places = jnp.arange(number_of)

    def named(sizes, turn):
        used = int((sizes > 0).sum())
        fixed = max(1, used // 4)
        shifted = fixed + (places - fixed + turn * (used - fixed)) % max(1, number_of - fixed)
        return jnp.zeros((number_of,), jnp.int32).at[ranking[jnp.where(places < fixed, places, shifted)]].set(jnp.asarray(sizes, jnp.int32))

    sizes = jnp.where(number % 4 == 0, named(packed, number // 4), named(usual, number - number // 4 - 1))
    mixed = jax.random.permutation(jax.random.fold_in(own, 3), number_of)
    source_of, sink = mixed[0:number_of // 2 * 2:2], mixed[1:number_of // 2 * 2:2]
    margin = jnp.minimum(sizes[source_of] - 1, bound - sizes[sink]) // 2
    margin = jnp.where((source_of == ranking[0]) | (sink == ranking[0]) | (sizes[sink] == 0), 0, jnp.maximum(margin, 0))
    shifted = jax.random.randint(jax.random.fold_in(own, 4), (number_of // 2,), 0, 1 << 20) % (margin + 1)
    sizes = sizes.at[source_of].add(-shifted).at[sink].add(shifted)
    items = jnp.searchsorted(jnp.cumsum(sizes), jnp.arange(rows * top), side="right").astype(jnp.int32)
    table = items.reshape(top, rows).T
    table = table[jax.random.permutation(jax.random.fold_in(own, 1), rows)]
    turn = jax.random.randint(jax.random.fold_in(own, 2), (rows, 1), 0, top)
    return jnp.take_along_axis(table, (jnp.arange(top)[None, :] + turn) % top, axis=1)


def load_shares(count, total, bound, lean, full):
    loads = [(1 << 20) // math.isqrt(rank ** lean) + 1 for rank in range(1, count + 1)]
    largest = bound if full else min(bound, max(-(-total // count), total * loads[0] // sum(loads)))
    least = 1 if total - largest >= count - 1 else 0
    given, surplus = [largest] + [least] * (count - 1), total - largest - least * (count - 1)
    while surplus > 0:
        candidates = [i for i in range(1, count) if given[i] < largest] or [i for i in range(1, count) if given[i] < bound]
        mass, remaining = sum([loads[i] for i in candidates]), surplus
        for i in candidates:
            extra = min(bound - given[i], max(1, remaining * loads[i] // mass), surplus)
            given[i] = given[i] + extra
            surplus = surplus - extra
    return np.array(given)


def bell_draw(rng, shape, deviation, most, shards=(), kind=jnp.bfloat16):
    entries = jax.random.normal(rng, shape, jnp.float32) * deviation
    if len(shards) > 0:
        entries = block_scale(rng, shape, shards, -0.22, 0.18) * entries
    return jnp.clip(entries, min=-most, max=most).astype(kind)


def setup_inputs(seed: int = 0) -> dict:
    keys = jax.random.split(jax.random.key(seed), 9)
    trajectory = bell_draw(keys[0], (NT, NB, G, LEV), 1.0, 6.0, ((0, 16), (1, 16)))
    weights = bell_draw(keys[1], (NGRP_ALL, CAPB, G), G ** -0.5, 0.375, ((0, 256),))
    observed = bell_draw(keys[2], (NGRP_ALL, CAPB, LEV), 1.5, 9.0, ((0, 256),))
    window_keys = jax.random.split(jax.random.fold_in(keys[3], 1), NGRP_ALL // NGRP)
    window_turns = jax.random.permutation(jax.random.fold_in(keys[3], 3), NGRP_ALL // NGRP)
    window = jax.vmap(lambda own, number: shared_out(jax.random.fold_in(keys[3], 2), own, number, NGRP, NT, 1, GCAP, 2))(window_keys, window_turns).reshape((NGRP_ALL, 1))
    block = place_ends(jax.random.randint(keys[4], (NGRP_ALL,), 0, BL), jax.random.fold_in(keys[4], 1), 0, BL - 1).astype(jnp.int32)
    counts = draw_counts(jax.random.fold_in(keys[8], 71), 0)
    flags = place_ends((jax.random.randint(keys[6], (NGRP_ALL, CAPB), 0, 4) < 3).astype(jnp.int32), jax.random.fold_in(keys[6], 1), 0, 1)
    inv_error = jnp.clip(jnp.exp(jax.random.uniform(keys[7], (LEV,), jnp.float32, math.log(0.5), math.log(2.0))), 0.5, 2.0)
    return {"trajectory": trajectory, "weights": weights, "observed": observed, "window": window, "block": block, "counts": counts, "flags": flags, "inv_error": inv_error}


def reference(trajectory, weights, observed, window, block, counts, flags, inv_error):
    devices = N_TM * N_OBS
    nwin = N_TM
    w_dev = weights.reshape(devices, NGRP, CAPB, G)
    y_dev = observed.reshape(devices, NGRP, CAPB, LEV)
    win_dev = window.reshape(devices, NGRP).astype(jnp.int32)
    blk_dev = block.reshape(devices, NGRP).astype(jnp.int32)
    cnt_dev = counts.reshape(devices, NGRP).astype(jnp.int32)
    flg_dev = flags.reshape(devices, NGRP, CAPB).astype(jnp.int32)
    dev_ids = jnp.arange(devices, dtype=jnp.int32)

    def one_device(items):
        dev, w_here, y_here, win_here, blk_here, cnt_here, flg_here = items
        region = (dev % N_OBS).astype(jnp.int32)
        slab = lax.dynamic_slice_in_dim(trajectory, region * BL, BL, 1)
        picked = slab[win_here, blk_here].astype(jnp.float32)
        hx = jnp.einsum('gop,gpl->gol', w_here.astype(jnp.float32), picked)
        slot_ids = jnp.arange(CAPB, dtype=jnp.int32)
        used = jnp.where(slot_ids[None, :] < cnt_here[:, None], flg_here, 0).astype(jnp.float32)
        departure = used[:, :, None] * (y_here.astype(jnp.float32) - hx) * inv_error[None, None, :]
        member = (win_here[:, None] == jnp.arange(nwin, dtype=jnp.int32)[None, :]).astype(jnp.float32)
        sum_one = jnp.einsum('gt,gl->tl', member, lax.optimization_barrier(jnp.sum(departure, 1)), precision=lax.Precision.HIGHEST)
        sum_two = jnp.einsum('gt,gl->tl', member, lax.optimization_barrier(jnp.sum(departure * departure, 1)), precision=lax.Precision.HIGHEST)
        kept = jnp.einsum('gt,g->t', member, lax.optimization_barrier(jnp.sum(used, 1)), precision=lax.Precision.HIGHEST)
        return (departure.astype(jnp.bfloat16), sum_one, sum_two, kept)
    deps, ones, twos, kepts = lax.map(one_device, (dev_ids, w_dev, y_dev, win_dev, blk_dev, cnt_dev, flg_dev))
    sum_one = lax.optimization_barrier(jnp.sum(ones, 0))
    sum_two = lax.optimization_barrier(jnp.sum(twos, 0))
    kept = lax.optimization_barrier(jnp.sum(kepts, 0))
    departures = deps.reshape(NGRP * devices, CAPB, LEV)
    window_bias = sum_one / jnp.sqrt(kept[:, None] + 1.0)
    window_chi = sum_two / (kept[:, None] + 1.0)
    return (departures, window_bias, window_chi)
```

```python
import jax
import jax.numpy as jnp
from jax import lax
from jax.experimental import pallas as pl
from jax.experimental.pallas import tpu as pltpu
from jax.sharding import PartitionSpec as P

MESH = pl.DeviceIdType.MESH
GCAP = 4
PIECE = 2

SLABS = ((0, 0), (-1, 0), (1, 0), (-2, 0), (2, 0))
TABLE_TO = ((0, 1), (-1, 0), (-1, 1), (-2, 0), (1, 0), (1, 1), (2, 1))
PICKS = (
    (0, 1, 0, 0),
    (0, 1, 1, 0),
    (0, 1, 2, 0),
    (0, 1, 3, 0),
    (0, 1, 4, 0),
    (1, 0, 3, 1),
    (1, 1, 3, 2),
    (2, 0, 3, 3),
    (-1, 0, 4, 4),
    (-1, 1, 4, 5),
    (-2, 1, 4, 6),
)


def kernel(
    traj, weights, observed, window, block, counts, flags, inv,
    dep_out, bias_out, chi_out,
    s0, s1, s2, s3, s4, picked, outgoing, w_all, y_all, deps, dep_rows, used_t, my_table, tables,
    parts, from_tm, row_sum, from_obs, my_smem, far_smem,
    load_sem, slab_send, slab_recv, pick_send, pick_recv, table_send, table_recv,
    tm_send, tm_recv, obs_send, obs_recv, out_sem,
):
    slabs = (s0, s1, s2, s3, s4)
    tm = lax.axis_index("tm")
    obs = lax.axis_index("obs")
    z, y = tm // 2, lax.rem(tm, 2)
    n_tm, n_obs = 16, 16
    groups = 32

    def at(dz, dy):
        return lax.rem(z + dz + 8, 8) * 2 + (1 - y if dy else y)

    loads = [
        pltpu.make_async_copy(traj.at[0], s0, load_sem.at[0]),
        pltpu.make_async_copy(weights, w_all, load_sem.at[1]),
        pltpu.make_async_copy(observed, y_all, load_sem.at[2]),
    ]
    for load in loads:
        load.start()

    barrier = pltpu.get_barrier_semaphore()

    def greet(step, carry):
        pl.semaphore_signal(
            barrier, 1, device_id={"tm": lax.rem(tm + step, n_tm)}, device_id_type=MESH
        )
        pl.semaphore_signal(
            barrier, 1, device_id={"obs": lax.rem(obs + step, n_obs)}, device_id_type=MESH
        )
        return carry

    lax.fori_loop(1, 16, greet, 0)

    lane = lax.broadcasted_iota(jnp.int32, (groups, 128), 1)
    row = lax.broadcasted_iota(jnp.int32, (groups, 128), 0)
    win_col = jnp.broadcast_to(window[...], (groups, 128))
    diag = lane == row
    win_row = jnp.sum(jnp.where(diag, win_col, 0), 0, keepdims=True)
    same = win_col == win_row
    rank_row = jnp.sum(jnp.where(same & (row < lane), 1, 0), 0, keepdims=True)
    slot_row = win_row * GCAP + rank_row
    rank_col = jnp.sum(jnp.where(same & (lane < row), 1, 0), 1, keepdims=True)
    slot_col = window[...] * GCAP + rank_col
    hit = slot_col == lane
    block_row = block[...]
    block_col = jnp.sum(
        jnp.where(diag, jnp.broadcast_to(block_row, (groups, 128)), 0), 1, keepdims=True
    )
    my_table[0:1, :] = jnp.sum(jnp.where(hit, block_col, 0), 0, keepdims=True)
    my_table[1:2, :] = jnp.sum(jnp.where(hit, row + 1, 0), 0, keepdims=True) - 1
    my_table[2:3, :] = slot_row
    count_col = jnp.sum(
        jnp.where(diag, jnp.broadcast_to(counts[...], (groups, 128)), 0), 1, keepdims=True
    )
    used = jnp.where(lane < count_col, flags[...], 0).astype(jnp.float32)
    used_t[...] = jnp.transpose(used).astype(jnp.bfloat16)

    loads[0].wait()
    pl.semaphore_wait(barrier, 2 * 15)

    pieces = 16 // PIECE

    def slab_copy(flow, piece):
        source, target, dz = ((s0, s1, 1), (s0, s2, -1), (s1, s3, 1), (s2, s4, -1))[flow]
        span = pl.ds(piece * PIECE, PIECE)
        return pltpu.make_async_remote_copy(
            src_ref=source.at[span], dst_ref=target.at[span],
            send_sem=slab_send.at[flow, piece], recv_sem=slab_recv.at[flow, piece],
            device_id={"tm": at(dz, 0)}, device_id_type=MESH,
        )

    def table_copy(k):
        return pltpu.make_async_remote_copy(
            src_ref=my_table, dst_ref=tables.at[k],
            send_sem=table_send.at[k], recv_sem=table_recv.at[k],
            device_id={"tm": at(*TABLE_TO[k])}, device_id_type=MESH,
        )

    for k in range(len(TABLE_TO)):
        table_copy(k).start()
    for piece in range(pieces):
        slab_copy(0, piece).start()
        slab_copy(1, piece).start()

    to_smem = pltpu.make_async_copy(my_table, my_smem, load_sem.at[3])
    to_smem.start()
    for k in range(len(TABLE_TO)):
        table_copy(k).wait_recv()
    far_to_smem = pltpu.make_async_copy(tables, far_smem, load_sem.at[4])
    far_to_smem.start()
    to_smem.wait()
    far_to_smem.wait()

    def pick_copy(m):
        dz, dy, _, _ = PICKS[m]
        return pltpu.make_async_remote_copy(
            src_ref=outgoing.at[m], dst_ref=picked.at[m],
            send_sem=pick_send.at[m], recv_sem=pick_recv.at[m],
            device_id={"tm": at(dz, dy)}, device_id_type=MESH,
        )

    def pick(*numbers):
        for m in numbers:
            _, _, slab, k = PICKS[m]
            first = at(*SLABS[slab]) * GCAP
            for r in range(GCAP):
                outgoing[m, r] = slabs[slab][far_smem[k, 0, first + r]]
        for m in numbers:
            pick_copy(m).start()

    inv_row = inv[...]
    group_ids = lax.broadcasted_iota(jnp.int32, (groups, 128), 0)
    done = []

    def part_copy(q, dz, dy):
        return pltpu.make_async_remote_copy(
            src_ref=parts.at[q], dst_ref=from_tm.at[q],
            send_sem=tm_send.at[q], recv_sem=tm_recv.at[q],
            device_id={"tm": at(dz, dy)}, device_id_type=MESH,
        )

    def send_part():
        q, dz, dy = done[-1]
        if q > 0:
            part_copy(q, dz, dy).start()

    def compute(dz, dy, block_of):
        q = len(done)
        first = at(dz, dy) * GCAP

        def body(r, carry):
            one, two, kept = carry
            group = my_smem[1, first + r]
            place = jnp.maximum(group, 0)
            chosen = jnp.where(group_ids == group, 1.0, 0.0).astype(jnp.bfloat16)
            mask = jnp.dot(used_t[...], chosen, preferred_element_type=jnp.float32)
            hx = jnp.dot(
                w_all[place], block_of(r, my_smem[0, first + r]), preferred_element_type=jnp.float32
            )
            departure = mask * (y_all[place].astype(jnp.float32) - hx) * inv_row
            deps[first + r] = departure.astype(jnp.bfloat16)
            one = one + jnp.sum(departure.reshape(16, 8, 128), 0)
            two = two + jnp.sum((departure * departure).reshape(16, 8, 128), 0)
            kept = kept + jnp.sum(mask.reshape(16, 8, 128), 0)
            return one, two, kept

        zero = jnp.zeros((8, 128), jnp.float32)
        one, two, kept = lax.fori_loop(0, GCAP, body, (zero, zero, zero))
        parts[q, 0:1, :] = jnp.sum(one, 0, keepdims=True)
        parts[q, 1:2, :] = jnp.sum(two, 0, keepdims=True)
        parts[q, 2:3, :] = jnp.sum(kept, 0, keepdims=True)
        if done:
            send_part()
        done.append((q, dz, dy))

    def compute_slab(slab):
        dz, dy = SLABS[slab]
        compute(dz, dy, lambda r, number: slabs[slab][number])

    def compute_picked(m):
        dz, dy, slab, _ = PICKS[m]
        compute(SLABS[slab][0] - dz, dy, lambda r, number: picked[m, r])

    pick(0)
    loads[1].wait()
    loads[2].wait()
    parts[...] = jnp.zeros_like(parts)
    compute_slab(0)

    for piece in range(pieces):
        slab_copy(0, piece).wait_recv()
        slab_copy(2, piece).start()
        slab_copy(1, piece).wait_recv()
        slab_copy(3, piece).start()
    pick(1, 2)
    pick_copy(0).wait_recv()
    compute_picked(0)
    compute_slab(1)
    compute_slab(2)
    pick_copy(1).wait_recv()
    compute_picked(1)
    pick_copy(2).wait_recv()
    compute_picked(2)

    for piece in range(pieces):
        slab_copy(2, piece).wait_recv()
        slab_copy(3, piece).wait_recv()
    pick(6, 9, 7, 10, 5, 8)
    pick(3, 4)
    compute_slab(3)
    compute_slab(4)
    for m in (6, 9, 7, 10, 5, 8, 3, 4):
        pick_copy(m).wait_recv()
        compute_picked(m)

    def put(lo, hi):
        for g in range(lo, hi):
            dep_rows[g] = deps[my_smem[2, g]]

    def out_copy(lo, size):
        span = pl.ds(lo, size)
        return pltpu.make_async_copy(dep_rows.at[span], dep_out.at[span], out_sem.at[lo // size])

    put(0, 4)
    send_part()
    put(4, 16)
    out_copy(0, 16).start()
    total = parts[0]
    for q, dz, dy in done[1:]:
        part_copy(q, dz, dy).wait_recv()
        total = total + from_tm[q]
    row_sum[...] = total
    put(16, 20)

    def obs_copy(step):
        return pltpu.make_async_remote_copy(
            src_ref=row_sum, dst_ref=from_obs.at[step],
            send_sem=obs_send.at[step], recv_sem=obs_recv.at[step],
            device_id={"obs": lax.rem(obs + step, n_obs)}, device_id_type=MESH,
        )

    for step in range(1, n_obs):
        obs_copy(step).start()
    put(20, 32)
    out_copy(16, 16).start()

    for piece in range(pieces):
        for flow in range(4):
            slab_copy(flow, piece).wait_send()
    for k in range(len(TABLE_TO)):
        table_copy(k).wait_send()
    for m in range(len(PICKS)):
        pick_copy(m).wait_send()
    for q, dz, dy in done[1:]:
        part_copy(q, dz, dy).wait_send()

    for step in range(1, n_obs):
        obs_copy(step).wait_recv()
        total = total + from_obs[step]
    plus_one = total[2:3, :] + 1.0
    bias_out[...] = total[0:1, :] / jnp.sqrt(plus_one)
    chi_out[...] = total[1:2, :] / plus_one
    for step in range(1, n_obs):
        obs_copy(step).wait_send()
    out_copy(0, 16).wait()
    out_copy(16, 16).wait()


def per_device(trajectory, weights, observed, window, block, counts, flags, inv_error):
    groups, slots, columns = weights.shape
    levels = observed.shape[2]
    blocks = trajectory.shape[1]
    bf16, f32, i32 = jnp.bfloat16, jnp.float32, jnp.int32
    pad = ((0, 0), (0, 128 - groups))
    block = jnp.pad(block.reshape(1, groups), pad)
    counts = jnp.pad(counts.reshape(1, groups), pad)
    dma = pltpu.SemaphoreType.DMA
    pieces = blocks // PIECE
    picks, tables = len(PICKS), len(TABLE_TO)
    any_space = pl.BlockSpec(memory_space=pl.ANY)
    hbm = pl.BlockSpec(memory_space=pltpu.HBM)
    vmem = pl.BlockSpec(memory_space=pltpu.VMEM)
    slab = pltpu.VMEM((blocks, columns, levels), bf16)
    return pl.pallas_call(
        kernel,
        out_shape=(
            jax.ShapeDtypeStruct((groups, slots, levels), bf16),
            jax.ShapeDtypeStruct((1, levels), f32),
            jax.ShapeDtypeStruct((1, levels), f32),
        ),
        in_specs=[hbm] * 3 + [vmem] * 5,
        out_specs=(any_space, vmem, vmem),
        scratch_shapes=[
            slab, slab, slab, slab, slab,
            pltpu.VMEM((picks, GCAP, columns, levels), bf16),
            pltpu.VMEM((picks, GCAP, columns, levels), bf16),
            pltpu.VMEM((groups, slots, columns), bf16),
            pltpu.VMEM((groups, slots, levels), bf16),
            pltpu.VMEM((16 * GCAP, slots, levels), bf16),
            pltpu.VMEM((groups, slots, levels), bf16),
            pltpu.VMEM((slots, groups), bf16),
            pltpu.VMEM((8, 128), i32),
            pltpu.VMEM((tables, 8, 128), i32),
            pltpu.VMEM((16, 8, levels), f32),
            pltpu.VMEM((16, 8, levels), f32),
            pltpu.VMEM((8, levels), f32),
            pltpu.VMEM((16, 8, levels), f32),
            pltpu.SMEM((8, 128), i32),
            pltpu.SMEM((tables, 8, 128), i32),
            dma((5,)),
            dma((4, pieces)), dma((4, pieces)),
            dma((picks,)), dma((picks,)),
            dma((tables,)), dma((tables,)),
            dma((16,)), dma((16,)),
            dma((16,)), dma((16,)),
            dma((2,)),
        ],
        compiler_params=pltpu.CompilerParams(
            collective_id=0, has_side_effects=True, vmem_limit_bytes=48 * 2**20
        ),
        name="exchange_and_check",
    )(
        trajectory, weights, observed, window, block, counts, flags,
        inv_error.reshape(1, levels),
    )


def solution(mesh):
    both = ("tm", "obs")
    return jax.shard_map(
        per_device,
        mesh=mesh,
        in_specs=(
            P("tm", "obs", None, None),
            P(both, None, None),
            P(both, None, None),
            P(both, None),
            P(both),
            P(both),
            P(both, None),
            P(),
        ),
        out_specs=(P(both, None, None), P("tm", None), P("tm", None)),
        check_vma=False,
    )
```

```python
import jax
import jax.numpy as jnp
from jax import lax
from jax.experimental import pallas as pl
from jax.experimental.pallas import tpu as pltpu
from jax.sharding import PartitionSpec as P

MESH = pl.DeviceIdType.MESH
GCAP = 4
PIECE = 2

SLABS = ((0, 0), (-1, 0), (1, 0), (-2, 0), (2, 0))
TABLE_TO = ((0, 1), (-1, 0), (-1, 1), (-2, 0), (1, 0), (1, 1), (2, 1))
PICKS = (
    (0, 1, 0, 0),
    (0, 1, 1, 0),
    (0, 1, 2, 0),
    (0, 1, 3, 0),
    (0, 1, 4, 0),
    (1, 0, 3, 1),
    (1, 1, 3, 2),
    (2, 0, 3, 3),
    (-1, 0, 4, 4),
    (-1, 1, 4, 5),
    (-2, 1, 4, 6),
)


def kernel(
    traj, weights, observed, window, block, counts, flags, inv,
    dep_out, sums_out,
    s0, s1, s2, s3, s4, picked, outgoing, w_all, y_all, deps, dep_rows, used_t,
    win_row, block_row, count_row, flag_rows, inv_vmem, my_table, tables,
    parts, from_tm, row_sum, from_obs, my_smem, far_smem,
    load_sem, slab_send, slab_recv, pick_send, pick_recv, table_send, table_recv,
    tm_send, tm_recv, obs_send, obs_recv, out_sem,
):
    slabs = (s0, s1, s2, s3, s4)
    tm = lax.axis_index("tm")
    obs = lax.axis_index("obs")
    z, y = tm // 2, lax.rem(tm, 2)
    n_tm, n_obs = 16, 16
    groups = 32

    def at(dz, dy):
        return lax.rem(z + dz + 8, 8) * 2 + (1 - y if dy else y)

    barrier = pltpu.get_barrier_semaphore()

    def greet(step, carry):
        pl.semaphore_signal(
            barrier, 1, device_id={"tm": lax.rem(tm + step, n_tm)}, device_id_type=MESH
        )
        pl.semaphore_signal(
            barrier, 1, device_id={"obs": lax.rem(obs + step, n_obs)}, device_id_type=MESH
        )
        return carry

    lax.fori_loop(1, 16, greet, 0)

    pairs = (
        (traj.at[0], s0), (weights, w_all), (observed, y_all), (window, win_row), (block, block_row),
        (counts, count_row), (flags, flag_rows), (inv, inv_vmem),
    )
    loads = [
        pltpu.make_async_copy(source, target, load_sem.at[n])
        for n, (source, target) in enumerate(pairs)
    ]
    for load in loads[3:] + loads[:3]:
        load.start()

    for load in loads[3:]:
        load.wait()
    lane = lax.broadcasted_iota(jnp.int32, (groups, groups), 1)
    row = lax.broadcasted_iota(jnp.int32, (groups, groups), 0)
    diag = lane == row

    def turned(ref):
        return jnp.sum(jnp.where(diag, ref[...], 0), 1, keepdims=True)

    same = turned(win_row) == win_row[...]
    rank_row = jnp.sum(jnp.where(same & (row < lane), 1, 0), 0, keepdims=True)
    rank_col = jnp.sum(jnp.where(same & (lane < row), 1, 0), 1, keepdims=True)
    wide_lane = lax.broadcasted_iota(jnp.int32, (groups, 128), 1)
    wide_row = lax.broadcasted_iota(jnp.int32, (groups, 128), 0)
    hit = turned(win_row) * GCAP + rank_col == wide_lane
    my_table[...] = jnp.zeros_like(my_table)
    my_table[0:1, :] = jnp.sum(jnp.where(hit, turned(block_row), 0), 0, keepdims=True)
    my_table[1:2, :] = jnp.sum(jnp.where(hit, wide_row + 1, 0), 0, keepdims=True) - 1
    my_table[2:3, 0:groups] = win_row[...] * GCAP + rank_row
    used = jnp.where(wide_lane < turned(count_row), flag_rows[...], 0).astype(jnp.float32)
    used_t[...] = jnp.transpose(used).astype(jnp.bfloat16)

    loads[0].wait()
    pl.semaphore_wait(barrier, 2 * 15)

    pieces = 16 // PIECE

    def slab_copy(flow, piece):
        source, target, dz = ((s0, s1, 1), (s0, s2, -1), (s1, s3, 1), (s2, s4, -1))[flow]
        span = pl.ds(piece * PIECE, PIECE)
        return pltpu.make_async_remote_copy(
            src_ref=source.at[span], dst_ref=target.at[span],
            send_sem=slab_send.at[flow, piece], recv_sem=slab_recv.at[flow, piece],
            device_id={"tm": at(dz, 0)}, device_id_type=MESH,
        )

    def table_copy(k):
        return pltpu.make_async_remote_copy(
            src_ref=my_table, dst_ref=tables.at[k],
            send_sem=table_send.at[k], recv_sem=table_recv.at[k],
            device_id={"tm": at(*TABLE_TO[k])}, device_id_type=MESH,
        )

    for k in range(len(TABLE_TO)):
        table_copy(k).start()
    for piece in range(pieces):
        slab_copy(0, piece).start()
        slab_copy(1, piece).start()

    to_smem = pltpu.make_async_copy(my_table, my_smem, load_sem.at[8])
    to_smem.start()
    for k in range(len(TABLE_TO)):
        table_copy(k).wait_recv()
    far_to_smem = pltpu.make_async_copy(tables, far_smem, load_sem.at[9])
    far_to_smem.start()
    to_smem.wait()
    far_to_smem.wait()

    def pick_copy(m):
        dz, dy, _, _ = PICKS[m]
        return pltpu.make_async_remote_copy(
            src_ref=outgoing.at[m], dst_ref=picked.at[m],
            send_sem=pick_send.at[m], recv_sem=pick_recv.at[m],
            device_id={"tm": at(dz, dy)}, device_id_type=MESH,
        )

    def pick(*numbers):
        for m in numbers:
            _, _, slab, k = PICKS[m]
            first = at(*SLABS[slab]) * GCAP
            for r in range(GCAP):
                outgoing[m, r] = slabs[slab][far_smem[k, 0, first + r]]
        for m in numbers:
            pick_copy(m).start()

    inv_row = inv_vmem[...]
    group_ids = lax.broadcasted_iota(jnp.int32, (groups, 128), 0)
    done = []

    def part_copy(q, dz, dy):
        return pltpu.make_async_remote_copy(
            src_ref=parts.at[q], dst_ref=from_tm.at[q],
            send_sem=tm_send.at[q], recv_sem=tm_recv.at[q],
            device_id={"tm": at(dz, dy)}, device_id_type=MESH,
        )

    def send_part():
        q, dz, dy = done[-1]
        if q > 0:
            part_copy(q, dz, dy).start()

    def compute(dz, dy, block_of):
        q = len(done)
        first = at(dz, dy) * GCAP

        def body(r, carry):
            one, two, kept = carry
            group = my_smem[1, first + r]
            place = jnp.maximum(group, 0)
            chosen = jnp.where(group_ids == group, 1.0, 0.0).astype(jnp.bfloat16)
            mask = jnp.dot(used_t[...], chosen, preferred_element_type=jnp.float32)
            hx = jnp.dot(
                w_all[place], block_of(r, my_smem[0, first + r]), preferred_element_type=jnp.float32
            )
            departure = mask * (y_all[place].astype(jnp.float32) - hx) * inv_row
            deps[first + r] = departure.astype(jnp.bfloat16)
            one = one + jnp.sum(departure.reshape(16, 8, 128), 0)
            two = two + jnp.sum((departure * departure).reshape(16, 8, 128), 0)
            kept = kept + jnp.sum(mask.reshape(16, 8, 128), 0)
            return one, two, kept

        zero = jnp.zeros((8, 128), jnp.float32)
        one, two, kept = lax.fori_loop(0, GCAP, body, (zero, zero, zero))
        parts[q, 0:1, :] = jnp.sum(one, 0, keepdims=True)
        parts[q, 1:2, :] = jnp.sum(two, 0, keepdims=True)
        parts[q, 2:3, :] = jnp.sum(kept, 0, keepdims=True)
        if done:
            send_part()
        done.append((q, dz, dy))

    def compute_slab(slab):
        dz, dy = SLABS[slab]
        compute(dz, dy, lambda r, number: slabs[slab][number])

    def compute_picked(m):
        dz, dy, slab, _ = PICKS[m]
        compute(SLABS[slab][0] - dz, dy, lambda r, number: picked[m, r])

    pick(0)
    loads[1].wait()
    loads[2].wait()
    parts[...] = jnp.zeros_like(parts)
    compute_slab(0)

    for piece in range(pieces):
        slab_copy(0, piece).wait_recv()
        slab_copy(2, piece).start()
        slab_copy(1, piece).wait_recv()
        slab_copy(3, piece).start()
    pick(1, 2)
    pick_copy(0).wait_recv()
    compute_picked(0)
    compute_slab(1)
    compute_slab(2)
    pick_copy(1).wait_recv()
    compute_picked(1)
    pick_copy(2).wait_recv()
    compute_picked(2)

    for piece in range(pieces):
        slab_copy(2, piece).wait_recv()
        slab_copy(3, piece).wait_recv()
    pick(6, 9, 7, 10, 5, 8)
    pick(3, 4)
    compute_slab(3)
    compute_slab(4)
    for m in (6, 9, 7, 10, 5, 8, 3, 4):
        pick_copy(m).wait_recv()
        compute_picked(m)

    def put(lo, hi):
        for g in range(lo, hi):
            dep_rows[g] = deps[my_smem[2, g]]

    def out_copy(lo, size):
        span = pl.ds(lo, size)
        return pltpu.make_async_copy(dep_rows.at[span], dep_out.at[span], out_sem.at[lo // size])

    put(0, 4)
    send_part()
    put(4, 16)
    out_copy(0, 16).start()
    total = parts[0]
    for q, dz, dy in done[1:]:
        part_copy(q, dz, dy).wait_recv()
        total = total + from_tm[q]
    row_sum[...] = total
    put(16, 20)

    def obs_copy(step):
        return pltpu.make_async_remote_copy(
            src_ref=row_sum, dst_ref=from_obs.at[step],
            send_sem=obs_send.at[step], recv_sem=obs_recv.at[step],
            device_id={"obs": lax.rem(obs + step, n_obs)}, device_id_type=MESH,
        )

    for step in range(1, n_obs):
        obs_copy(step).start()
    put(20, 32)
    out_copy(16, 16).start()

    for piece in range(pieces):
        for flow in range(4):
            slab_copy(flow, piece).wait_send()
    for k in range(len(TABLE_TO)):
        table_copy(k).wait_send()
    for m in range(len(PICKS)):
        pick_copy(m).wait_send()
    for q, dz, dy in done[1:]:
        part_copy(q, dz, dy).wait_send()

    for step in range(1, n_obs):
        obs_copy(step).wait_recv()
        total = total + from_obs[step]
    sums_out[...] = total
    for step in range(1, n_obs):
        obs_copy(step).wait_send()
    out_copy(0, 16).wait()
    out_copy(16, 16).wait()


def per_device(trajectory, weights, observed, window, block, counts, flags, inv_error):
    groups, slots, columns = weights.shape
    levels = observed.shape[2]
    blocks = trajectory.shape[1]
    bf16, f32, i32 = jnp.bfloat16, jnp.float32, jnp.int32
    dma = pltpu.SemaphoreType.DMA
    pieces = blocks // PIECE
    picks, tables = len(PICKS), len(TABLE_TO)
    any_space = pl.BlockSpec(memory_space=pl.ANY)
    vmem = pl.BlockSpec(memory_space=pltpu.VMEM)
    slab = pltpu.VMEM((blocks, columns, levels), bf16)
    departures, sums = pl.pallas_call(
        kernel,
        out_shape=(
            jax.ShapeDtypeStruct((groups, slots, levels), bf16),
            jax.ShapeDtypeStruct((8, levels), f32),
        ),
        in_specs=[any_space] * 8,
        out_specs=(any_space, vmem),
        scratch_shapes=[
            slab, slab, slab, slab, slab,
            pltpu.VMEM((picks, GCAP, columns, levels), bf16),
            pltpu.VMEM((picks, GCAP, columns, levels), bf16),
            pltpu.VMEM((groups, slots, columns), bf16),
            pltpu.VMEM((groups, slots, levels), bf16),
            pltpu.VMEM((16 * GCAP, slots, levels), bf16),
            pltpu.VMEM((groups, slots, levels), bf16),
            pltpu.VMEM((slots, groups), bf16),
            pltpu.VMEM((1, groups), i32),
            pltpu.VMEM((1, groups), i32),
            pltpu.VMEM((1, groups), i32),
            pltpu.VMEM((groups, slots), i32),
            pltpu.VMEM((1, levels), f32),
            pltpu.VMEM((8, 128), i32),
            pltpu.VMEM((tables, 8, 128), i32),
            pltpu.VMEM((16, 8, levels), f32),
            pltpu.VMEM((16, 8, levels), f32),
            pltpu.VMEM((8, levels), f32),
            pltpu.VMEM((16, 8, levels), f32),
            pltpu.SMEM((8, 128), i32),
            pltpu.SMEM((tables, 8, 128), i32),
            dma((10,)),
            dma((4, pieces)), dma((4, pieces)),
            dma((picks,)), dma((picks,)),
            dma((tables,)), dma((tables,)),
            dma((16,)), dma((16,)),
            dma((16,)), dma((16,)),
            dma((2,)),
        ],
        compiler_params=pltpu.CompilerParams(
            collective_id=0, has_side_effects=True, vmem_limit_bytes=67043328
        ),
        name="exchange_and_check",
    )(
        trajectory, weights, observed, window.reshape(1, groups), block.reshape(1, groups),
        counts.reshape(1, groups), flags, inv_error.reshape(1, levels),
    )
    plus_one = sums[2:3] + 1.0
    return departures, sums[0:1] / jnp.sqrt(plus_one), sums[1:2] / plus_one


def solution(mesh):
    both = ("tm", "obs")
    return jax.shard_map(
        per_device,
        mesh=mesh,
        in_specs=(
            P("tm", "obs", None, None),
            P(both, None, None),
            P(both, None, None),
            P(both, None),
            P(both),
            P(both),
            P(both, None),
            P(),
        ),
        out_specs=(P(both, None, None), P("tm", None), P("tm", None)),
        check_vma=False,
    )
```

```python
import jax
import jax.numpy as jnp
from jax import lax
from jax.experimental import pallas as pl
from jax.experimental.pallas import tpu as pltpu
from jax.sharding import PartitionSpec as P

MESH = pl.DeviceIdType.MESH
GCAP = 4
PIECE = 2

SLABS = ((0, 0), (-1, 0), (1, 0), (-2, 0), (2, 0), (2, 1))
FLOWS = ((0, 1, 1, 0), (0, 2, -1, 0), (1, 3, 1, 0), (2, 4, -1, 0), (4, 5, 0, 1))
PIECE_SEM = {0: 0, 1: 16 // PIECE, 3: 2 * (16 // PIECE)}
TABLE_TO = ((0, 1), (-1, 0), (-1, 1), (-2, 0), (1, 0), (2, 0))
PICKS = (
    (0, 1, 0, 0),
    (0, 1, 1, 0),
    (0, 1, 2, 0),
    (0, 1, 3, 0),
    (1, 0, 3, 1),
    (1, 1, 3, 2),
    (2, 0, 3, 3),
    (-1, 0, 4, 4),
    (-1, 0, 5, 4),
    (-2, 0, 5, 5),
)


def kernel(
    traj, weights, observed, window, block, counts, flags, inv,
    dep_out, sums_out,
    s0, s1, s2, s3, s4, s5, picked, outgoing, w_all, y_all, deps, used_t,
    win_row, block_row, count_row, flag_rows, inv_vmem, my_table, tables,
    parts, from_tm, row_sum, from_obs, my_smem, far_smem,
    load_sem, slab_send, slab_recv, whole_recv, pick_send, pick_recv, table_send, table_recv,
    tm_send, tm_recv, obs_send, obs_recv,
):
    slabs = (s0, s1, s2, s3, s4, s5)
    tm = lax.axis_index("tm")
    obs = lax.axis_index("obs")
    z, y = tm // 2, lax.rem(tm, 2)
    n_obs = 16
    groups = 32

    def at(dz, dy):
        return lax.rem(z + dz + 8, 8) * 2 + (1 - y if dy else y)

    barrier = pltpu.get_barrier_semaphore()

    for dz, dy in ((-1, 0), (1, 0), (0, 1)):
        pl.semaphore_signal(barrier, 1, device_id={"tm": at(dz, dy)}, device_id_type=MESH)

    def greet(step, carry):
        pl.semaphore_signal(
            barrier, 1, device_id={"obs": lax.rem(obs + step, n_obs)}, device_id_type=MESH
        )
        return carry

    lax.fori_loop(1, 16, greet, 0)

    pairs = (
        (traj.at[0], s0), (weights, w_all), (observed, y_all), (window, win_row), (block, block_row),
        (counts, count_row), (flags, flag_rows), (inv, inv_vmem),
    )
    loads = [
        pltpu.make_async_copy(source, target, load_sem.at[n])
        for n, (source, target) in enumerate(pairs)
    ]
    for load in loads[3:] + loads[:3]:
        load.start()

    for load in loads[3:]:
        load.wait()
    lane = lax.broadcasted_iota(jnp.int32, (groups, groups), 1)
    row = lax.broadcasted_iota(jnp.int32, (groups, groups), 0)
    diag = lane == row

    def turned(ref):
        return jnp.sum(jnp.where(diag, ref[...], 0), 1, keepdims=True)

    same = turned(win_row) == win_row[...]
    rank_row = jnp.sum(jnp.where(same & (row < lane), 1, 0), 0, keepdims=True)
    rank_col = jnp.sum(jnp.where(same & (lane < row), 1, 0), 1, keepdims=True)
    wide_lane = lax.broadcasted_iota(jnp.int32, (groups, 128), 1)
    wide_row = lax.broadcasted_iota(jnp.int32, (groups, 128), 0)
    hit = turned(win_row) * GCAP + rank_col == wide_lane
    my_table[...] = jnp.zeros_like(my_table)
    my_table[0:1, :] = jnp.sum(jnp.where(hit, turned(block_row), 0), 0, keepdims=True)
    my_table[1:2, :] = jnp.sum(jnp.where(hit, wide_row + 1, 0), 0, keepdims=True) - 1
    my_table[2:3, 0:groups] = win_row[...] * GCAP + rank_row
    used = jnp.where(wide_lane < turned(count_row), flag_rows[...], 0).astype(jnp.float32)
    used_t[...] = jnp.transpose(used).astype(jnp.bfloat16)

    loads[0].wait()
    pl.semaphore_wait(barrier, 3 + 15)

    pieces = 16 // PIECE

    def slab_copy(flow, piece):
        source, target, dz, dy = FLOWS[flow]
        span = pl.ds(piece * PIECE, PIECE)
        return pltpu.make_async_remote_copy(
            src_ref=slabs[source].at[span], dst_ref=slabs[target].at[span],
            send_sem=slab_send.at[flow], recv_sem=slab_recv.at[PIECE_SEM[flow] + piece] if flow in PIECE_SEM else whole_recv.at[flow // 2 - 1],
            device_id={"tm": at(dz, dy)}, device_id_type=MESH,
        )

    def all_of(flow):
        source, target, dz, dy = FLOWS[flow]
        return pltpu.make_async_remote_copy(
            src_ref=slabs[source], dst_ref=slabs[target],
            send_sem=slab_send.at[flow], recv_sem=whole_recv.at[max(flow // 2 - 1, 0)],
            device_id={"tm": at(dz, dy)}, device_id_type=MESH,
        )

    def table_copy(k):
        return pltpu.make_async_remote_copy(
            src_ref=my_table, dst_ref=tables.at[k],
            send_sem=table_send.at[0], recv_sem=table_recv.at[k],
            device_id={"tm": at(*TABLE_TO[k])}, device_id_type=MESH,
        )

    for k in (1, 4, 0):
        table_copy(k).start()
    for piece in range(pieces):
        slab_copy(0, piece).start()
        slab_copy(1, piece).start()

    to_smem = pltpu.make_async_copy(my_table, my_smem, load_sem.at[8])
    to_smem.start()
    table_copy(0).wait_recv()
    mate_to_smem = pltpu.make_async_copy(tables.at[0], far_smem.at[0], load_sem.at[9])
    mate_to_smem.start()
    to_smem.wait()
    mate_to_smem.wait()

    def pick_copy(m):
        dz, dy, _, _ = PICKS[m]
        return pltpu.make_async_remote_copy(
            src_ref=outgoing.at[m], dst_ref=picked.at[m],
            send_sem=pick_send.at[0], recv_sem=pick_recv.at[m],
            device_id={"tm": at(dz, dy)}, device_id_type=MESH,
        )

    def pick(m):
        _, _, slab, k = PICKS[m]
        first = at(*SLABS[slab]) * GCAP
        for r in range(GCAP):
            outgoing[m, r] = slabs[slab][far_smem[k, 0, first + r]]

    def send(*numbers):
        for m in numbers:
            pick(m)
            pick_copy(m).start()

    inv_row = inv_vmem[...]
    group_ids = lax.broadcasted_iota(jnp.int32, (groups, 128), 0)
    done = []

    def part_copy(q, dz, dy):
        return pltpu.make_async_remote_copy(
            src_ref=parts.at[q], dst_ref=from_tm.at[q],
            send_sem=tm_send.at[0], recv_sem=tm_recv.at[0],
            device_id={"tm": at(dz, dy)}, device_id_type=MESH,
        )

    def send_part():
        q, dz, dy = done[-1]
        if q > 0:
            part_copy(q, dz, dy).start()

    def compute(dz, dy, block_of):
        q = len(done)
        first = at(dz, dy) * GCAP

        def body(r, carry):
            one, two, kept = carry
            group = my_smem[1, first + r]
            place = jnp.maximum(group, 0)
            chosen = jnp.where(group_ids == group, 1.0, 0.0).astype(jnp.bfloat16)
            mask = jnp.dot(used_t[...], chosen, preferred_element_type=jnp.float32)
            hx = jnp.dot(
                w_all[place], block_of(r, my_smem[0, first + r]), preferred_element_type=jnp.float32
            )
            departure = mask * (y_all[place].astype(jnp.float32) - hx) * inv_row
            deps[first + r] = departure.astype(jnp.bfloat16)
            one = one + jnp.sum(departure.reshape(16, 8, 128), 0)
            two = two + jnp.sum((departure * departure).reshape(16, 8, 128), 0)
            kept = kept + jnp.sum(mask.reshape(16, 8, 128), 0)
            return one, two, kept

        zero = jnp.zeros((8, 128), jnp.float32)
        one, two, kept = lax.fori_loop(0, GCAP, body, (zero, zero, zero))
        parts[q, 0:1, :] = jnp.sum(one, 0, keepdims=True)
        parts[q, 1:2, :] = jnp.sum(two, 0, keepdims=True)
        parts[q, 2:3, :] = jnp.sum(kept, 0, keepdims=True)
        if done:
            send_part()
        done.append((q, dz, dy))

    def compute_slab(slab):
        dz, dy = SLABS[slab]
        compute(dz, dy, lambda r, number: slabs[slab][number])

    def compute_picked(m):
        dz, dy, slab, _ = PICKS[m]
        compute(SLABS[slab][0] - dz, dy ^ SLABS[slab][1], lambda r, number: picked[m, r])

    def receive(m):
        pick_copy(m).wait_recv()
        compute_picked(m)

    send(0)
    loads[1].wait()
    loads[2].wait()
    parts[...] = jnp.zeros_like(parts)
    compute_slab(0)
    table_copy(1).wait_recv()
    table_copy(4).wait_recv()
    for k in (2, 3, 5):
        table_copy(k).start()

    for piece in range(pieces):
        slab_copy(0, piece).wait_recv()
        slab_copy(2, piece).start()
        slab_copy(1, piece).wait_recv()
        slab_copy(3, piece).start()
    pick(1)
    pick(2)
    beside = [lambda: compute_slab(1), lambda: compute_slab(2), lambda: receive(0)]
    for piece in range(pieces):
        slab_copy(3, piece).wait_recv()
        slab_copy(4, piece).start()
        if beside:
            beside.pop(0)()
        if piece == pieces - 3:
            for k in (2, 3, 5):
                table_copy(k).wait_recv()
            rest = pl.ds(1, len(TABLE_TO) - 1)
            far_to_smem = pltpu.make_async_copy(
                tables.at[rest], far_smem.at[rest], load_sem.at[10]
            )
            far_to_smem.start()
    far_to_smem.wait()
    pick_copy(1).start()
    pick_copy(2).start()

    all_of(2).wait_recv()
    send(6, 7, 4, 5, 3)
    compute_slab(3)
    compute_slab(4)
    all_of(4).wait_recv()
    send(9, 8)
    compute_slab(5)
    for m in (1, 7, 6, 2, 3, 9, 4, 8, 5):
        receive(m)

    others = pl.ds(1, 15)

    def wait_bytes(ref, semaphore):
        pltpu.make_async_copy(ref, ref, semaphore).wait()

    def put(lo, hi):
        for g in range(lo, hi):
            dep_out[g] = deps[my_smem[2, g]]

    put(0, 4)
    send_part()
    put(4, 16)
    total = parts[0]
    wait_bytes(from_tm.at[others], tm_recv.at[0])
    for q in range(1, 16):
        total = total + from_tm[q]
    row_sum[...] = total
    put(16, 20)

    def obs_copy(step):
        return pltpu.make_async_remote_copy(
            src_ref=row_sum, dst_ref=from_obs.at[step],
            send_sem=obs_send.at[0], recv_sem=obs_recv.at[0],
            device_id={"obs": lax.rem(obs + step, n_obs)}, device_id_type=MESH,
        )

    for step in range(1, n_obs):
        obs_copy(step).start()
    put(20, 32)

    for flow in range(len(FLOWS)):
        all_of(flow).wait_send()
    wait_bytes(tables, table_send.at[0])
    wait_bytes(outgoing, pick_send.at[0])
    wait_bytes(from_tm.at[others], tm_send.at[0])

    wait_bytes(from_obs.at[others], obs_recv.at[0])
    for step in range(1, n_obs):
        total = total + from_obs[step]
    sums_out[...] = total
    wait_bytes(from_obs.at[others], obs_send.at[0])


def per_device(trajectory, weights, observed, window, block, counts, flags, inv_error):
    groups, slots, columns = weights.shape
    levels = observed.shape[2]
    blocks = trajectory.shape[1]
    bf16, f32, i32 = jnp.bfloat16, jnp.float32, jnp.int32
    dma = pltpu.SemaphoreType.DMA
    pieces = blocks // PIECE
    picks, tables = len(PICKS), len(TABLE_TO)
    any_space = pl.BlockSpec(memory_space=pl.ANY)
    vmem = pl.BlockSpec(memory_space=pltpu.VMEM)
    slab = pltpu.VMEM((blocks, columns, levels), bf16)
    arrays = (
        trajectory, weights, observed, window.reshape(1, groups), block.reshape(1, groups),
        counts.reshape(1, groups), flags, inv_error.reshape(1, levels),
    )
    departures, sums = pl.pallas_call(
        kernel,
        out_shape=(
            jax.ShapeDtypeStruct((groups, slots, levels), bf16),
            jax.ShapeDtypeStruct((8, levels), f32),
        ),
        in_specs=[any_space] * 8,
        out_specs=(vmem, vmem),
        scratch_shapes=[
            slab, slab, slab, slab, slab, slab,
            pltpu.VMEM((picks, GCAP, columns, levels), bf16),
            pltpu.VMEM((picks, GCAP, columns, levels), bf16),
            pltpu.VMEM((groups, slots, columns), bf16),
            pltpu.VMEM((groups, slots, levels), bf16),
            pltpu.VMEM((16 * GCAP, slots, levels), bf16),
            pltpu.VMEM((slots, groups), bf16),
            pltpu.VMEM((1, groups), i32),
            pltpu.VMEM((1, groups), i32),
            pltpu.VMEM((1, groups), i32),
            pltpu.VMEM((groups, slots), i32),
            pltpu.VMEM((1, levels), f32),
            pltpu.VMEM((8, 128), i32),
            pltpu.VMEM((tables, 8, 128), i32),
            pltpu.VMEM((16, 8, levels), f32),
            pltpu.VMEM((16, 8, levels), f32),
            pltpu.VMEM((8, levels), f32),
            pltpu.VMEM((16, 8, levels), f32),
            pltpu.SMEM((8, 128), i32),
            pltpu.SMEM((tables, 8, 128), i32),
            dma((11,)),
            dma((len(FLOWS),)), dma((3 * pieces,)), dma((2,)),
            dma((1,)), dma((picks,)),
            dma((1,)), dma((tables,)),
            dma((1,)), dma((1,)),
            dma((1,)), dma((1,)),
        ],
        compiler_params=pltpu.CompilerParams(
            collective_id=0, has_side_effects=True, vmem_limit_bytes=40 * 2**20
        ),
        name="exchange_and_check",
    )(*(pltpu.with_memory_space_constraint(array, pltpu.HBM) for array in arrays))
    plus_one = sums[2:3] + 1.0
    return departures, sums[0:1] / jnp.sqrt(plus_one), sums[1:2] / plus_one


def solution(mesh):
    both = ("tm", "obs")
    return jax.shard_map(
        per_device,
        mesh=mesh,
        in_specs=(
            P("tm", "obs", None, None),
            P(both, None, None),
            P(both, None, None),
            P(both, None),
            P(both),
            P(both),
            P(both, None),
            P(),
        ),
        out_specs=(P(both, None, None), P("tm", None), P("tm", None)),
        check_vma=False,
    )
```

```python
import jax
import jax.numpy as jnp
from jax import lax
from jax.experimental import pallas as pl
from jax.experimental.pallas import tpu as pltpu
from jax.sharding import PartitionSpec as P

MESH = pl.DeviceIdType.MESH
GCAP = 4
PIECE = 2
AHEAD = 3
LATE = 2

SLABS = ((0, 0), (-1, 0), (1, 0), (-2, 0), (2, 0), (2, 1))
FLOWS = ((0, 1, 1, 0), (0, 2, -1, 0), (1, 3, 1, 0), (2, 4, -1, 0), (4, 5, 0, 1))
PIECE_SEM = {0: 0, 1: 16 // PIECE, 3: 2 * (16 // PIECE)}
TABLE_TO = ((0, 1), (-1, 0), (-1, 1), (-2, 0), (1, 0), (2, 0))
PICKS = (
    (0, 1, 0, 0),
    (0, 1, 1, 0),
    (0, 1, 2, 0),
    (0, 1, 3, 0),
    (1, 0, 3, 1),
    (1, 1, 3, 2),
    (2, 0, 3, 3),
    (-1, 0, 4, 4),
    (-1, 0, 5, 4),
    (-2, 0, 5, 5),
)


def kernel(
    traj, weights, observed, window, block, counts, flags, inv,
    dep_out, sums_out,
    s0, s1, s2, s3, s4, s5, picked, outgoing, w_all, y_all, deps, used_t,
    win_row, block_row, count_row, flag_rows, inv_vmem, my_table, tables,
    parts, from_tm, row_sum, from_obs, from_late, my_smem, far_smem,
    load_sem, slab_send, slab_recv, whole_recv, pick_send, pick_recv, table_send, table_recv,
    tm_send, tm_recv, obs_send, obs_recv, late_send, late_recv,
):
    slabs = (s0, s1, s2, s3, s4, s5)
    tm = lax.axis_index("tm")
    obs = lax.axis_index("obs")
    z, y = tm // 2, lax.rem(tm, 2)
    n_obs = 16
    groups = 32

    def at(dz, dy):
        return lax.rem(z + dz + 8, 8) * 2 + (1 - y if dy else y)

    barrier = pltpu.get_barrier_semaphore()

    for dz, dy in ((-1, 0), (1, 0), (0, 1)):
        pl.semaphore_signal(barrier, 1, device_id={"tm": at(dz, dy)}, device_id_type=MESH)

    def greet(step, carry):
        pl.semaphore_signal(
            barrier, 1, device_id={"obs": lax.rem(obs + step, n_obs)}, device_id_type=MESH
        )
        return carry

    lax.fori_loop(1, 16, greet, 0)

    pairs = (
        (traj.at[0], s0), (weights, w_all), (observed, y_all), (window, win_row), (block, block_row),
        (counts, count_row), (flags, flag_rows), (inv, inv_vmem),
    )
    loads = [
        pltpu.make_async_copy(source, target, load_sem.at[n])
        for n, (source, target) in enumerate(pairs)
    ]
    for load in loads[3:] + loads[:3]:
        load.start()

    for load in loads[3:]:
        load.wait()
    lane = lax.broadcasted_iota(jnp.int32, (groups, groups), 1)
    row = lax.broadcasted_iota(jnp.int32, (groups, groups), 0)
    diag = lane == row

    def turned(ref):
        return jnp.sum(jnp.where(diag, ref[...], 0), 1, keepdims=True)

    same = turned(win_row) == win_row[...]
    rank_row = jnp.sum(jnp.where(same & (row < lane), 1, 0), 0, keepdims=True)
    rank_col = jnp.sum(jnp.where(same & (lane < row), 1, 0), 1, keepdims=True)
    wide_lane = lax.broadcasted_iota(jnp.int32, (groups, 128), 1)
    wide_row = lax.broadcasted_iota(jnp.int32, (groups, 128), 0)
    hit = turned(win_row) * GCAP + rank_col == wide_lane
    my_table[...] = jnp.zeros_like(my_table)
    my_table[0:1, :] = jnp.sum(jnp.where(hit, turned(block_row), 0), 0, keepdims=True)
    my_table[1:2, :] = jnp.sum(jnp.where(hit, wide_row + 1, 0), 0, keepdims=True) - 1
    my_table[2:3, 0:groups] = win_row[...] * GCAP + rank_row
    used = jnp.where(wide_lane < turned(count_row), flag_rows[...], 0).astype(jnp.float32)
    used_t[...] = jnp.transpose(used).astype(jnp.bfloat16)

    loads[0].wait()
    pl.semaphore_wait(barrier, 3 + 15)

    pieces = 16 // PIECE

    def slab_copy(flow, piece):
        source, target, dz, dy = FLOWS[flow]
        span = pl.ds(piece * PIECE, PIECE)
        return pltpu.make_async_remote_copy(
            src_ref=slabs[source].at[span], dst_ref=slabs[target].at[span],
            send_sem=slab_send.at[flow], recv_sem=slab_recv.at[PIECE_SEM[flow] + piece] if flow in PIECE_SEM else whole_recv.at[flow // 2 - 1],
            device_id={"tm": at(dz, dy)}, device_id_type=MESH,
        )

    def all_of(flow):
        source, target, dz, dy = FLOWS[flow]
        return pltpu.make_async_remote_copy(
            src_ref=slabs[source], dst_ref=slabs[target],
            send_sem=slab_send.at[flow], recv_sem=whole_recv.at[max(flow // 2 - 1, 0)],
            device_id={"tm": at(dz, dy)}, device_id_type=MESH,
        )

    def table_copy(k):
        return pltpu.make_async_remote_copy(
            src_ref=my_table, dst_ref=tables.at[k],
            send_sem=table_send.at[0], recv_sem=table_recv.at[k],
            device_id={"tm": at(*TABLE_TO[k])}, device_id_type=MESH,
        )

    for k in (1, 4, 0):
        table_copy(k).start()
    for piece in range(pieces):
        slab_copy(0, piece).start()
        if piece < AHEAD:
            slab_copy(1, piece).start()

    to_smem = pltpu.make_async_copy(my_table, my_smem, load_sem.at[8])
    to_smem.start()
    table_copy(0).wait_recv()
    mate_to_smem = pltpu.make_async_copy(tables.at[0], far_smem.at[0], load_sem.at[9])
    mate_to_smem.start()
    to_smem.wait()
    mate_to_smem.wait()

    def pick_copy(m):
        dz, dy, _, _ = PICKS[m]
        return pltpu.make_async_remote_copy(
            src_ref=outgoing.at[m], dst_ref=picked.at[m],
            send_sem=pick_send.at[0], recv_sem=pick_recv.at[m],
            device_id={"tm": at(dz, dy)}, device_id_type=MESH,
        )

    def pick(m):
        _, _, slab, k = PICKS[m]
        first = at(*SLABS[slab]) * GCAP
        for r in range(GCAP):
            outgoing[m, r] = slabs[slab][far_smem[k, 0, first + r]]

    def send(*numbers):
        for m in numbers:
            pick(m)
            pick_copy(m).start()

    inv_row = inv_vmem[...]
    group_ids = lax.broadcasted_iota(jnp.int32, (groups, 128), 0)
    done = []
    rows = pl.ds(0, 4)

    def part_copy(q, dz, dy):
        return pltpu.make_async_remote_copy(
            src_ref=parts.at[q, rows], dst_ref=from_tm.at[q, rows],
            send_sem=tm_send.at[0], recv_sem=tm_recv.at[0],
            device_id={"tm": at(dz, dy)}, device_id_type=MESH,
        )

    def late_copy(q, dz, dy, step):
        return pltpu.make_async_remote_copy(
            src_ref=parts.at[q, rows], dst_ref=from_late.at[q - (16 - LATE), step, rows],
            send_sem=late_send.at[0], recv_sem=late_recv.at[0],
            device_id={"tm": at(dz, dy), "obs": lax.rem(obs + step, n_obs)}, device_id_type=MESH,
        )

    def send_part():
        q, dz, dy = done[-1]
        if q >= 16 - LATE:
            for step in range(n_obs):
                late_copy(q, dz, dy, step).start()
        elif q > 0:
            part_copy(q, dz, dy).start()

    def compute(dz, dy, block_of):
        q = len(done)
        first = at(dz, dy) * GCAP

        def body(r, carry):
            one, two, kept = carry
            group = my_smem[1, first + r]
            place = jnp.maximum(group, 0)
            chosen = jnp.where(group_ids == group, 1.0, 0.0).astype(jnp.bfloat16)
            mask = jnp.dot(used_t[...], chosen, preferred_element_type=jnp.float32)
            hx = jnp.dot(
                w_all[place], block_of(r, my_smem[0, first + r]), preferred_element_type=jnp.float32
            )
            departure = mask * (y_all[place].astype(jnp.float32) - hx) * inv_row
            deps[first + r] = departure.astype(jnp.bfloat16)
            one = one + jnp.sum(departure.reshape(16, 8, 128), 0)
            two = two + jnp.sum((departure * departure).reshape(16, 8, 128), 0)
            kept = kept + jnp.sum(mask.reshape(16, 8, 128), 0)
            return one, two, kept

        zero = jnp.zeros((8, 128), jnp.float32)
        one, two, kept = lax.fori_loop(0, GCAP, body, (zero, zero, zero))
        parts[q, 0:1, :] = jnp.sum(one, 0, keepdims=True)
        parts[q, 1:2, :] = jnp.sum(two, 0, keepdims=True)
        parts[q, 2:3, :] = jnp.sum(kept, 0, keepdims=True)
        if done:
            send_part()
        done.append((q, dz, dy))

    def compute_slab(slab):
        dz, dy = SLABS[slab]
        compute(dz, dy, lambda r, number: slabs[slab][number])

    def compute_picked(m):
        dz, dy, slab, _ = PICKS[m]
        compute(SLABS[slab][0] - dz, dy ^ SLABS[slab][1], lambda r, number: picked[m, r])

    def receive(m):
        pick_copy(m).wait_recv()
        compute_picked(m)

    def forward_up(*numbers):
        for piece in numbers:
            slab_copy(0, piece).wait_recv()
            slab_copy(2, piece).start()

    def forward_down(piece):
        slab_copy(1, piece).wait_recv()
        slab_copy(3, piece).start()
        if piece + AHEAD < pieces:
            slab_copy(1, piece + AHEAD).start()

    def cross(piece):
        slab_copy(3, piece).wait_recv()
        slab_copy(4, piece).start()

    send(0)
    forward_down(0)
    loads[1].wait()
    loads[2].wait()
    parts[...] = jnp.zeros_like(parts)
    compute_slab(0)
    forward_down(1)
    table_copy(1).wait_recv()
    table_copy(4).wait_recv()
    for k in (2, 3, 5):
        table_copy(k).start()
    forward_up(0, 1)
    forward_down(2)
    forward_up(2)
    cross(0)
    forward_up(3)
    forward_down(3)
    forward_up(4)
    cross(1)
    forward_up(5)
    forward_down(4)
    forward_up(6, 7)
    send(1)
    cross(2)
    compute_slab(1)
    forward_down(5)
    receive(0)
    cross(3)
    forward_down(6)
    cross(4)
    forward_down(7)
    send(2)
    compute_slab(2)
    cross(5)
    for k in (2, 3, 5):
        table_copy(k).wait_recv()
    rest = pl.ds(1, len(TABLE_TO) - 1)
    far_to_smem = pltpu.make_async_copy(tables.at[rest], far_smem.at[rest], load_sem.at[10])
    far_to_smem.start()
    cross(6)
    cross(7)
    far_to_smem.wait()

    all_of(2).wait_recv()
    send(6, 7, 4, 5, 3)
    compute_slab(3)
    compute_slab(4)
    all_of(4).wait_recv()
    send(9, 8)
    compute_slab(5)
    for m in (1, 2, 7, 3, 6, 9, 4, 8, 5):
        receive(m)

    others = pl.ds(1, 15)
    early = pl.ds(1, 15 - LATE)

    def wait_bytes(ref, semaphore):
        pltpu.make_async_copy(ref, ref, semaphore).wait()

    def put(lo, hi):
        for g in range(lo, hi):
            dep_out[g] = deps[my_smem[2, g]]

    put(0, 4)
    send_part()
    put(4, 16)
    total = parts[0]
    wait_bytes(from_tm.at[early, rows], tm_recv.at[0])
    for q in range(1, 16 - LATE):
        total = total + from_tm[q]
    row_sum[...] = total
    put(16, 20)

    def obs_copy(step):
        return pltpu.make_async_remote_copy(
            src_ref=row_sum.at[rows], dst_ref=from_obs.at[step, rows],
            send_sem=obs_send.at[0], recv_sem=obs_recv.at[0],
            device_id={"obs": lax.rem(obs + step, n_obs)}, device_id_type=MESH,
        )

    for step in range(1, n_obs):
        obs_copy(step).start()
    put(20, 32)

    for flow in range(len(FLOWS)):
        all_of(flow).wait_send()
    wait_bytes(tables, table_send.at[0])
    wait_bytes(outgoing, pick_send.at[0])
    wait_bytes(from_tm.at[early, rows], tm_send.at[0])

    wait_bytes(from_obs.at[others, rows], obs_recv.at[0])
    for step in range(1, n_obs):
        total = total + from_obs[step]
    wait_bytes(from_late.at[pl.ds(0, LATE), pl.ds(0, n_obs), rows], late_recv.at[0])
    for number in range(LATE):
        for step in range(n_obs):
            total = total + from_late[number, step]
    sums_out[...] = total
    wait_bytes(from_obs.at[others, rows], obs_send.at[0])
    wait_bytes(from_late.at[pl.ds(0, LATE), pl.ds(0, n_obs), rows], late_send.at[0])


def per_device(trajectory, weights, observed, window, block, counts, flags, inv_error):
    groups, slots, columns = weights.shape
    levels = observed.shape[2]
    blocks = trajectory.shape[1]
    bf16, f32, i32 = jnp.bfloat16, jnp.float32, jnp.int32
    dma = pltpu.SemaphoreType.DMA
    pieces = blocks // PIECE
    picks, tables = len(PICKS), len(TABLE_TO)
    any_space = pl.BlockSpec(memory_space=pl.ANY)
    vmem = pl.BlockSpec(memory_space=pltpu.VMEM)
    slab = pltpu.VMEM((blocks, columns, levels), bf16)
    arrays = (
        trajectory, weights, observed, window.reshape(1, groups), block.reshape(1, groups),
        counts.reshape(1, groups), flags, inv_error.reshape(1, levels),
    )
    departures, sums = pl.pallas_call(
        kernel,
        out_shape=(
            jax.ShapeDtypeStruct((groups, slots, levels), bf16),
            jax.ShapeDtypeStruct((8, levels), f32),
        ),
        in_specs=[any_space] * 8,
        out_specs=(vmem, vmem),
        scratch_shapes=[
            slab, slab, slab, slab, slab, slab,
            pltpu.VMEM((picks, GCAP, columns, levels), bf16),
            pltpu.VMEM((picks, GCAP, columns, levels), bf16),
            pltpu.VMEM((groups, slots, columns), bf16),
            pltpu.VMEM((groups, slots, levels), bf16),
            pltpu.VMEM((16 * GCAP, slots, levels), bf16),
            pltpu.VMEM((slots, groups), bf16),
            pltpu.VMEM((1, groups), i32),
            pltpu.VMEM((1, groups), i32),
            pltpu.VMEM((1, groups), i32),
            pltpu.VMEM((groups, slots), i32),
            pltpu.VMEM((1, levels), f32),
            pltpu.VMEM((8, 128), i32),
            pltpu.VMEM((tables, 8, 128), i32),
            pltpu.VMEM((16, 8, levels), f32),
            pltpu.VMEM((16, 8, levels), f32),
            pltpu.VMEM((8, levels), f32),
            pltpu.VMEM((16, 8, levels), f32),
            pltpu.VMEM((LATE, 16, 8, levels), f32),
            pltpu.SMEM((8, 128), i32),
            pltpu.SMEM((tables, 8, 128), i32),
            dma((11,)),
            dma((len(FLOWS),)), dma((3 * pieces,)), dma((2,)),
            dma((1,)), dma((picks,)),
            dma((1,)), dma((tables,)),
            dma((1,)), dma((1,)),
            dma((1,)), dma((1,)),
            dma((1,)), dma((1,)),
        ],
        compiler_params=pltpu.CompilerParams(
            collective_id=0, has_side_effects=True, vmem_limit_bytes=40 * 2**20
        ),
        name="exchange_and_check",
    )(*(pltpu.with_memory_space_constraint(array, pltpu.HBM) for array in arrays))
    plus_one = sums[2:3] + 1.0
    return departures, sums[0:1] / jnp.sqrt(plus_one), sums[1:2] / plus_one


def solution(mesh):
    both = ("tm", "obs")
    return jax.shard_map(
        per_device,
        mesh=mesh,
        in_specs=(
            P("tm", "obs", None, None),
            P(both, None, None),
            P(both, None, None),
            P(both, None),
            P(both),
            P(both),
            P(both, None),
            P(),
        ),
        out_specs=(P(both, None, None), P("tm", None), P("tm", None)),
        check_vma=False,
    )
```

```python
import jax
import jax.numpy as jnp
from jax import lax
from jax.experimental import pallas as pl
from jax.experimental.pallas import tpu as pltpu
from jax.sharding import PartitionSpec as P

MESH = pl.DeviceIdType.MESH
GCAP = 4
PIECE = 2
AHEAD = 3
LATE = 2

SLABS = ((0, 0), (-1, 0), (1, 0), (-2, 0), (2, 0), (2, 1))
FLOWS = ((0, 1, 1, 0), (0, 2, -1, 0), (1, 3, 1, 0), (2, 4, -1, 0), (4, 5, 0, 1))
PIECE_SEM = {0: 0, 1: 16 // PIECE, 3: 2 * (16 // PIECE)}
TABLE_TO = ((0, 1), (-1, 0), (-1, 1), (-2, 0), (1, 0), (2, 0))
PICKS = (
    (0, 1, 0, 0),
    (0, 1, 1, 0),
    (0, 1, 2, 0),
    (0, 1, 3, 0),
    (1, 0, 3, 1),
    (1, 1, 3, 2),
    (2, 0, 3, 3),
    (-1, 0, 4, 4),
    (-1, 0, 5, 4),
    (-2, 0, 5, 5),
)


def kernel(
    traj, weights, observed, window, block, counts, flags, inv,
    dep_out, sums_out,
    s0, s1, s2, s3, s4, s5, picked, outgoing, w_all, y_all, deps, used_t,
    win_row, block_row, count_row, flag_rows, inv_vmem, my_table, tables,
    parts, from_tm, row_sum, from_obs, from_late, my_smem, far_smem,
    load_sem, slab_send, slab_recv, whole_recv, pick_send, pick_recv, table_send, table_recv,
    tm_send, tm_recv, obs_send, obs_recv, late_send, late_recv,
):
    slabs = (s0, s1, s2, s3, s4, s5)
    tm = lax.axis_index("tm")
    obs = lax.axis_index("obs")
    z, y = tm // 2, lax.rem(tm, 2)
    n_obs = 16
    groups = 32

    def at(dz, dy):
        return lax.rem(z + dz + 8, 8) * 2 + (1 - y if dy else y)

    barrier = pltpu.get_barrier_semaphore()

    for dz, dy in ((-1, 0), (1, 0), (0, 1)):
        pl.semaphore_signal(barrier, 1, device_id={"tm": at(dz, dy)}, device_id_type=MESH)

    def greet(step, carry):
        pl.semaphore_signal(
            barrier, 1, device_id={"obs": lax.rem(obs + step, n_obs)}, device_id_type=MESH
        )
        return carry

    lax.fori_loop(1, 16, greet, 0)

    pairs = (
        (traj.at[0], s0), (weights, w_all), (observed, y_all), (window, win_row), (block, block_row),
        (counts, count_row), (flags, flag_rows), (inv, inv_vmem),
    )
    loads = [
        pltpu.make_async_copy(source, target, load_sem.at[n])
        for n, (source, target) in enumerate(pairs)
    ]
    for load in loads[3:5] + loads[:1] + loads[5:] + loads[1:3]:
        load.start()

    for load in loads[3:5]:
        load.wait()
    lane = lax.broadcasted_iota(jnp.int32, (groups, groups), 1)
    row = lax.broadcasted_iota(jnp.int32, (groups, groups), 0)
    diag = lane == row

    def turned(ref):
        return jnp.sum(jnp.where(diag, ref[...], 0), 1, keepdims=True)

    same = turned(win_row) == win_row[...]
    rank_row = jnp.sum(jnp.where(same & (row < lane), 1, 0), 0, keepdims=True)
    rank_col = jnp.sum(jnp.where(same & (lane < row), 1, 0), 1, keepdims=True)
    wide_lane = lax.broadcasted_iota(jnp.int32, (groups, 128), 1)
    wide_row = lax.broadcasted_iota(jnp.int32, (groups, 128), 0)
    hit = turned(win_row) * GCAP + rank_col == wide_lane
    my_table[...] = jnp.zeros_like(my_table)
    my_table[0:1, :] = jnp.sum(jnp.where(hit, turned(block_row), 0), 0, keepdims=True)
    my_table[1:2, :] = jnp.sum(jnp.where(hit, wide_row + 1, 0), 0, keepdims=True) - 1
    my_table[2:3, 0:groups] = win_row[...] * GCAP + rank_row

    loads[0].wait()
    pl.semaphore_wait(barrier, 3 + 15)

    pieces = 16 // PIECE

    def slab_copy(flow, piece):
        source, target, dz, dy = FLOWS[flow]
        span = pl.ds(piece * PIECE, PIECE)
        return pltpu.make_async_remote_copy(
            src_ref=slabs[source].at[span], dst_ref=slabs[target].at[span],
            send_sem=slab_send.at[flow], recv_sem=slab_recv.at[PIECE_SEM[flow] + piece] if flow in PIECE_SEM else whole_recv.at[flow // 2 - 1],
            device_id={"tm": at(dz, dy)}, device_id_type=MESH,
        )

    def all_of(flow):
        source, target, dz, dy = FLOWS[flow]
        return pltpu.make_async_remote_copy(
            src_ref=slabs[source], dst_ref=slabs[target],
            send_sem=slab_send.at[flow], recv_sem=whole_recv.at[max(flow // 2 - 1, 0)],
            device_id={"tm": at(dz, dy)}, device_id_type=MESH,
        )

    def table_copy(k):
        return pltpu.make_async_remote_copy(
            src_ref=my_table, dst_ref=tables.at[k],
            send_sem=table_send.at[0], recv_sem=table_recv.at[k],
            device_id={"tm": at(*TABLE_TO[k])}, device_id_type=MESH,
        )

    for k in (1, 4, 0):
        table_copy(k).start()
    for piece in range(pieces):
        slab_copy(0, piece).start()
        if piece < AHEAD:
            slab_copy(1, piece).start()

    for load in loads[5:]:
        load.wait()
    used = jnp.where(wide_lane < turned(count_row), flag_rows[...], 0).astype(jnp.float32)
    used_t[...] = jnp.transpose(used).astype(jnp.bfloat16)
    to_smem = pltpu.make_async_copy(my_table, my_smem, load_sem.at[8])
    to_smem.start()
    table_copy(0).wait_recv()
    mate_to_smem = pltpu.make_async_copy(tables.at[0], far_smem.at[0], load_sem.at[9])
    mate_to_smem.start()
    to_smem.wait()
    mate_to_smem.wait()

    def pick_copy(m):
        dz, dy, _, _ = PICKS[m]
        return pltpu.make_async_remote_copy(
            src_ref=outgoing.at[m], dst_ref=picked.at[m],
            send_sem=pick_send.at[0], recv_sem=pick_recv.at[m],
            device_id={"tm": at(dz, dy)}, device_id_type=MESH,
        )

    def pick(m):
        _, _, slab, k = PICKS[m]
        first = at(*SLABS[slab]) * GCAP
        for r in range(GCAP):
            outgoing[m, r] = slabs[slab][far_smem[k, 0, first + r]]

    def send(*numbers):
        for m in numbers:
            pick(m)
            pick_copy(m).start()

    inv_row = inv_vmem[...]
    group_ids = lax.broadcasted_iota(jnp.int32, (groups, 128), 0)
    done = []
    rows = pl.ds(0, 4)

    def part_copy(q, dz, dy):
        return pltpu.make_async_remote_copy(
            src_ref=parts.at[q, rows], dst_ref=from_tm.at[q, rows],
            send_sem=tm_send.at[0], recv_sem=tm_recv.at[0],
            device_id={"tm": at(dz, dy)}, device_id_type=MESH,
        )

    def late_copy(q, dz, dy, step):
        return pltpu.make_async_remote_copy(
            src_ref=parts.at[q, rows], dst_ref=from_late.at[q - (16 - LATE), step, rows],
            send_sem=late_send.at[0], recv_sem=late_recv.at[0],
            device_id={"tm": at(dz, dy), "obs": lax.rem(obs + step, n_obs)}, device_id_type=MESH,
        )

    def send_part():
        q, dz, dy = done[-1]
        if q >= 16 - LATE:
            for step in range(n_obs):
                late_copy(q, dz, dy, step).start()
        elif q > 0:
            part_copy(q, dz, dy).start()

    def compute(dz, dy, block_of):
        q = len(done)
        first = at(dz, dy) * GCAP

        def body(r, carry):
            one, two, kept = carry
            group = my_smem[1, first + r]
            place = jnp.maximum(group, 0)
            chosen = jnp.where(group_ids == group, 1.0, 0.0).astype(jnp.bfloat16)
            mask = jnp.dot(used_t[...], chosen, preferred_element_type=jnp.float32)
            hx = jnp.dot(
                w_all[place], block_of(r, my_smem[0, first + r]), preferred_element_type=jnp.float32
            )
            departure = mask * (y_all[place].astype(jnp.float32) - hx) * inv_row
            deps[first + r] = departure.astype(jnp.bfloat16)
            one = one + jnp.sum(departure.reshape(16, 8, 128), 0)
            two = two + jnp.sum((departure * departure).reshape(16, 8, 128), 0)
            kept = kept + jnp.sum(mask.reshape(16, 8, 128), 0)
            return one, two, kept

        zero = jnp.zeros((8, 128), jnp.float32)
        one, two, kept = lax.fori_loop(0, GCAP, body, (zero, zero, zero))
        parts[q, 0:1, :] = jnp.sum(one, 0, keepdims=True)
        parts[q, 1:2, :] = jnp.sum(two, 0, keepdims=True)
        parts[q, 2:3, :] = jnp.sum(kept, 0, keepdims=True)
        if done:
            send_part()
        done.append((q, dz, dy))

    def compute_slab(slab):
        dz, dy = SLABS[slab]
        compute(dz, dy, lambda r, number: slabs[slab][number])

    def compute_picked(m):
        dz, dy, slab, _ = PICKS[m]
        compute(SLABS[slab][0] - dz, dy ^ SLABS[slab][1], lambda r, number: picked[m, r])

    def receive(m):
        pick_copy(m).wait_recv()
        compute_picked(m)

    def forward_up(*numbers):
        for piece in numbers:
            slab_copy(0, piece).wait_recv()
            slab_copy(2, piece).start()

    def forward_down(piece):
        slab_copy(1, piece).wait_recv()
        slab_copy(3, piece).start()
        if piece + AHEAD < pieces:
            slab_copy(1, piece + AHEAD).start()

    def cross(piece):
        slab_copy(3, piece).wait_recv()
        slab_copy(4, piece).start()

    send(0)
    forward_down(0)
    loads[1].wait()
    loads[2].wait()
    parts[...] = jnp.zeros_like(parts)
    compute_slab(0)
    forward_down(1)
    table_copy(1).wait_recv()
    table_copy(4).wait_recv()
    for k in (2, 3, 5):
        table_copy(k).start()
    forward_up(0, 1)
    forward_down(2)
    forward_up(2)
    cross(0)
    forward_up(3)
    forward_down(3)
    forward_up(4)
    cross(1)
    forward_up(5)
    forward_down(4)
    forward_up(6, 7)
    send(1)
    cross(2)
    compute_slab(1)
    forward_down(5)
    receive(0)
    cross(3)
    forward_down(6)
    cross(4)
    forward_down(7)
    send(2)
    compute_slab(2)
    cross(5)
    for k in (2, 3, 5):
        table_copy(k).wait_recv()
    rest = pl.ds(1, len(TABLE_TO) - 1)
    far_to_smem = pltpu.make_async_copy(tables.at[rest], far_smem.at[rest], load_sem.at[10])
    far_to_smem.start()
    cross(6)
    cross(7)
    far_to_smem.wait()

    all_of(2).wait_recv()
    send(6, 7, 4, 5, 3)
    compute_slab(3)
    compute_slab(4)
    all_of(4).wait_recv()
    send(9, 8)
    compute_slab(5)
    for m in (1, 2, 7, 6, 3, 9, 4, 5, 8):
        receive(m)

    others = pl.ds(1, 15)
    early = pl.ds(1, 15 - LATE)

    def wait_bytes(ref, semaphore):
        pltpu.make_async_copy(ref, ref, semaphore).wait()

    def put(lo, hi):
        for g in range(lo, hi):
            dep_out[g] = deps[my_smem[2, g]]

    put(0, 4)
    send_part()
    put(4, 16)
    total = parts[0]
    wait_bytes(from_tm.at[early, rows], tm_recv.at[0])
    for q in range(1, 16 - LATE):
        total = total + from_tm[q]
    row_sum[...] = total
    put(16, 20)

    def obs_copy(step):
        return pltpu.make_async_remote_copy(
            src_ref=row_sum.at[rows], dst_ref=from_obs.at[step, rows],
            send_sem=obs_send.at[0], recv_sem=obs_recv.at[0],
            device_id={"obs": lax.rem(obs + step, n_obs)}, device_id_type=MESH,
        )

    for step in range(1, n_obs):
        obs_copy(step).start()
    put(20, 32)

    for flow in range(len(FLOWS)):
        all_of(flow).wait_send()
    wait_bytes(tables, table_send.at[0])
    wait_bytes(outgoing, pick_send.at[0])
    wait_bytes(from_tm.at[early, rows], tm_send.at[0])

    wait_bytes(from_obs.at[others, rows], obs_recv.at[0])
    for step in range(1, n_obs):
        total = total + from_obs[step]
    wait_bytes(from_late.at[pl.ds(0, LATE), pl.ds(0, n_obs), rows], late_recv.at[0])
    for number in range(LATE):
        for step in range(n_obs):
            total = total + from_late[number, step]
    sums_out[...] = total
    wait_bytes(from_obs.at[others, rows], obs_send.at[0])
    wait_bytes(from_late.at[pl.ds(0, LATE), pl.ds(0, n_obs), rows], late_send.at[0])


def per_device(trajectory, weights, observed, window, block, counts, flags, inv_error):
    groups, slots, columns = weights.shape
    levels = observed.shape[2]
    blocks = trajectory.shape[1]
    bf16, f32, i32 = jnp.bfloat16, jnp.float32, jnp.int32
    dma = pltpu.SemaphoreType.DMA
    pieces = blocks // PIECE
    picks, tables = len(PICKS), len(TABLE_TO)
    any_space = pl.BlockSpec(memory_space=pl.ANY)
    vmem = pl.BlockSpec(memory_space=pltpu.VMEM)
    slab = pltpu.VMEM((blocks, columns, levels), bf16)
    arrays = (
        trajectory, weights, observed, window.reshape(1, groups), block.reshape(1, groups),
        counts.reshape(1, groups), flags, inv_error.reshape(1, levels),
    )
    departures, sums = pl.pallas_call(
        kernel,
        out_shape=(
            jax.ShapeDtypeStruct((groups, slots, levels), bf16),
            jax.ShapeDtypeStruct((8, levels), f32),
        ),
        in_specs=[any_space] * 8,
        out_specs=(vmem, vmem),
        scratch_shapes=[
            slab, slab, slab, slab, slab, slab,
            pltpu.VMEM((picks, GCAP, columns, levels), bf16),
            pltpu.VMEM((picks, GCAP, columns, levels), bf16),
            pltpu.VMEM((groups, slots, columns), bf16),
            pltpu.VMEM((groups, slots, levels), bf16),
            pltpu.VMEM((16 * GCAP, slots, levels), bf16),
            pltpu.VMEM((slots, groups), bf16),
            pltpu.VMEM((1, groups), i32),
            pltpu.VMEM((1, groups), i32),
            pltpu.VMEM((1, groups), i32),
            pltpu.VMEM((groups, slots), i32),
            pltpu.VMEM((1, levels), f32),
            pltpu.VMEM((8, 128), i32),
            pltpu.VMEM((tables, 8, 128), i32),
            pltpu.VMEM((16, 8, levels), f32),
            pltpu.VMEM((16, 8, levels), f32),
            pltpu.VMEM((8, levels), f32),
            pltpu.VMEM((16, 8, levels), f32),
            pltpu.VMEM((LATE, 16, 8, levels), f32),
            pltpu.SMEM((8, 128), i32),
            pltpu.SMEM((tables, 8, 128), i32),
            dma((11,)),
            dma((len(FLOWS),)), dma((3 * pieces,)), dma((2,)),
            dma((1,)), dma((picks,)),
            dma((1,)), dma((tables,)),
            dma((1,)), dma((1,)),
            dma((1,)), dma((1,)),
            dma((1,)), dma((1,)),
        ],
        compiler_params=pltpu.CompilerParams(
            collective_id=0, has_side_effects=True, vmem_limit_bytes=40 * 2**20
        ),
        name="exchange_and_check",
    )(*(pltpu.with_memory_space_constraint(array, pltpu.HBM) for array in arrays))
    plus_one = sums[2:3] + 1.0
    return departures, sums[0:1] / jnp.sqrt(plus_one), sums[1:2] / plus_one


def solution(mesh):
    both = ("tm", "obs")
    return jax.shard_map(
        per_device,
        mesh=mesh,
        in_specs=(
            P("tm", "obs", None, None),
            P(both, None, None),
            P(both, None, None),
            P(both, None),
            P(both),
            P(both),
            P(both, None),
            P(),
        ),
        out_specs=(P(both, None, None), P("tm", None), P("tm", None)),
        check_vma=False,
    )
```

```python
import jax
import jax.numpy as jnp
from jax import lax
from jax.experimental import pallas as pl
from jax.experimental.pallas import tpu as pltpu
from jax.sharding import PartitionSpec as P

MESH = pl.DeviceIdType.MESH
GCAP = 4
PIECE = 2
AHEAD = 3
LATE = 2

SLABS = ((0, 0), (-1, 0), (1, 0), (-2, 0), (2, 0), (2, 1))
FLOWS = ((0, 1, 1, 0), (0, 2, -1, 0), (1, 3, 1, 0), (2, 4, -1, 0), (4, 5, 0, 1))
PIECE_SEM = {0: 0, 1: 16 // PIECE, 3: 2 * (16 // PIECE)}
TABLE_TO = ((0, 1), (-1, 0), (-1, 1), (-2, 0), (1, 0), (2, 0))
PICKS = (
    (0, 1, 0, 0),
    (0, 1, 1, 0),
    (0, 1, 2, 0),
    (0, 1, 3, 0),
    (1, 0, 3, 1),
    (1, 1, 3, 2),
    (2, 0, 3, 3),
    (-1, 0, 4, 4),
    (-1, 0, 5, 4),
    (-2, 0, 5, 5),
)


def kernel(
    traj, weights, observed, window, block, counts, flags, inv,
    dep_out, sums_out,
    s0, s1, s2, s3, s4, s5, picked, outgoing, w_all, y_all, deps, used_t,
    win_row, block_row, count_row, flag_rows, inv_vmem, my_table, tables,
    parts, from_tm, row_sum, from_obs, from_late, my_smem, far_smem,
    load_sem, slab_send, slab_recv, whole_recv, pick_send, pick_recv, table_send, table_recv,
    tm_send, tm_recv, obs_send, obs_recv, late_send, late_recv,
):
    slabs = (s0, s1, s2, s3, s4, s5)
    tm = lax.axis_index("tm")
    obs = lax.axis_index("obs")
    z, y = tm // 2, lax.rem(tm, 2)
    n_obs = 16
    groups = 32

    def at(dz, dy):
        return lax.rem(z + dz + 8, 8) * 2 + (1 - y if dy else y)

    barrier = pltpu.get_barrier_semaphore()

    for dz, dy in ((-1, 0), (1, 0), (0, 1)):
        pl.semaphore_signal(barrier, 1, device_id={"tm": at(dz, dy)}, device_id_type=MESH)

    def greet(step, carry):
        pl.semaphore_signal(
            barrier, 1, device_id={"obs": lax.rem(obs + step, n_obs)}, device_id_type=MESH
        )
        return carry

    lax.fori_loop(1, 16, greet, 0)

    pairs = (
        (traj.at[0], s0), (weights, w_all), (observed, y_all), (window, win_row), (block, block_row),
        (counts, count_row), (flags, flag_rows), (inv, inv_vmem),
    )
    loads = [
        pltpu.make_async_copy(source, target, load_sem.at[n])
        for n, (source, target) in enumerate(pairs)
    ]
    for load in loads[3:5] + loads[:1] + loads[5:] + loads[1:3]:
        load.start()

    for load in loads[3:5]:
        load.wait()
    lane = lax.broadcasted_iota(jnp.int32, (groups, groups), 1)
    row = lax.broadcasted_iota(jnp.int32, (groups, groups), 0)
    diag = lane == row

    def turned(ref):
        return jnp.sum(jnp.where(diag, ref[...], 0), 1, keepdims=True)

    same = turned(win_row) == win_row[...]
    rank_row = jnp.sum(jnp.where(same & (row < lane), 1, 0), 0, keepdims=True)
    rank_col = jnp.sum(jnp.where(same & (lane < row), 1, 0), 1, keepdims=True)
    wide_lane = lax.broadcasted_iota(jnp.int32, (groups, 128), 1)
    wide_row = lax.broadcasted_iota(jnp.int32, (groups, 128), 0)
    hit = turned(win_row) * GCAP + rank_col == wide_lane
    my_table[...] = jnp.zeros_like(my_table)
    my_table[0:1, :] = jnp.sum(jnp.where(hit, turned(block_row), 0), 0, keepdims=True)
    my_table[1:2, :] = jnp.sum(jnp.where(hit, wide_row + 1, 0), 0, keepdims=True) - 1
    my_table[2:3, 0:groups] = win_row[...] * GCAP + rank_row

    loads[0].wait()
    pl.semaphore_wait(barrier, 3 + 15)

    pieces = 16 // PIECE

    def slab_copy(flow, piece):
        source, target, dz, dy = FLOWS[flow]
        span = pl.ds(piece * PIECE, PIECE)
        return pltpu.make_async_remote_copy(
            src_ref=slabs[source].at[span], dst_ref=slabs[target].at[span],
            send_sem=slab_send.at[flow], recv_sem=slab_recv.at[PIECE_SEM[flow] + piece] if flow in PIECE_SEM else whole_recv.at[flow // 2 - 1],
            device_id={"tm": at(dz, dy)}, device_id_type=MESH,
        )

    def all_of(flow):
        source, target, dz, dy = FLOWS[flow]
        return pltpu.make_async_remote_copy(
            src_ref=slabs[source], dst_ref=slabs[target],
            send_sem=slab_send.at[flow], recv_sem=whole_recv.at[max(flow // 2 - 1, 0)],
            device_id={"tm": at(dz, dy)}, device_id_type=MESH,
        )

    def table_copy(k):
        return pltpu.make_async_remote_copy(
            src_ref=my_table, dst_ref=tables.at[k],
            send_sem=table_send.at[0], recv_sem=table_recv.at[k],
            device_id={"tm": at(*TABLE_TO[k])}, device_id_type=MESH,
        )

    for k in (1, 4, 0):
        table_copy(k).start()
    for piece in range(pieces):
        slab_copy(0, piece).start()
        if piece < AHEAD:
            slab_copy(1, piece).start()

    for load in loads[5:]:
        load.wait()
    used = jnp.where(wide_lane < turned(count_row), flag_rows[...], 0).astype(jnp.float32)
    used_t[...] = jnp.transpose(used).astype(jnp.bfloat16)
    to_smem = pltpu.make_async_copy(my_table, my_smem, load_sem.at[8])
    to_smem.start()
    table_copy(0).wait_recv()
    mate_to_smem = pltpu.make_async_copy(tables.at[0], far_smem.at[0], load_sem.at[9])
    mate_to_smem.start()
    to_smem.wait()
    mate_to_smem.wait()

    def pick_copy(m):
        dz, dy, _, _ = PICKS[m]
        return pltpu.make_async_remote_copy(
            src_ref=outgoing.at[m], dst_ref=picked.at[m],
            send_sem=pick_send.at[0], recv_sem=pick_recv.at[m],
            device_id={"tm": at(dz, dy)}, device_id_type=MESH,
        )

    def pick(m):
        _, _, slab, k = PICKS[m]
        first = at(*SLABS[slab]) * GCAP
        for r in range(GCAP):
            outgoing[m, r] = slabs[slab][far_smem[k, 0, first + r]]

    def send(*numbers):
        for m in numbers:
            pick(m)
            pick_copy(m).start()

    inv_row = inv_vmem[...]
    group_ids = lax.broadcasted_iota(jnp.int32, (groups, 128), 0)
    done = []
    rows = pl.ds(0, 4)

    def part_copy(q, dz, dy):
        return pltpu.make_async_remote_copy(
            src_ref=parts.at[q, rows], dst_ref=from_tm.at[q, rows],
            send_sem=tm_send.at[0], recv_sem=tm_recv.at[0],
            device_id={"tm": at(dz, dy)}, device_id_type=MESH,
        )

    def late_copy(q, dz, dy, step):
        return pltpu.make_async_remote_copy(
            src_ref=parts.at[q, rows], dst_ref=from_late.at[q - (16 - LATE), step, rows],
            send_sem=late_send.at[0], recv_sem=late_recv.at[0],
            device_id={"tm": at(dz, dy), "obs": lax.rem(obs + step, n_obs)}, device_id_type=MESH,
        )

    def send_part():
        q, dz, dy = done[-1]
        if q >= 16 - LATE:
            for step in range(n_obs):
                late_copy(q, dz, dy, step).start()
        elif q > 0:
            part_copy(q, dz, dy).start()

    def compute(dz, dy, block_of):
        q = len(done)
        first = at(dz, dy) * GCAP

        def body(r, carry):
            one, two, kept = carry
            group = my_smem[1, first + r]
            place = jnp.maximum(group, 0)
            chosen = jnp.where(group_ids == group, 1.0, 0.0).astype(jnp.bfloat16)
            mask = jnp.dot(used_t[...], chosen, preferred_element_type=jnp.float32)
            hx = jnp.dot(
                w_all[place], block_of(r, my_smem[0, first + r]), preferred_element_type=jnp.float32
            )
            departure = mask * (y_all[place].astype(jnp.float32) - hx) * inv_row
            deps[first + r] = departure.astype(jnp.bfloat16)
            one = one + jnp.sum(departure.reshape(16, 8, 128), 0)
            two = two + jnp.sum((departure * departure).reshape(16, 8, 128), 0)
            kept = kept + jnp.sum(mask.reshape(16, 8, 128), 0)
            return one, two, kept

        zero = jnp.zeros((8, 128), jnp.float32)
        one, two, kept = lax.fori_loop(0, GCAP, body, (zero, zero, zero), unroll=True)
        parts[q, 0:1, :] = jnp.sum(one, 0, keepdims=True)
        parts[q, 1:2, :] = jnp.sum(two, 0, keepdims=True)
        parts[q, 2:3, :] = jnp.sum(kept, 0, keepdims=True)
        if done:
            send_part()
        done.append((q, dz, dy))

    def compute_slab(slab):
        dz, dy = SLABS[slab]
        compute(dz, dy, lambda r, number: slabs[slab][number])

    def compute_picked(m):
        dz, dy, slab, _ = PICKS[m]
        compute(SLABS[slab][0] - dz, dy ^ SLABS[slab][1], lambda r, number: picked[m, r])

    def receive(m):
        pick_copy(m).wait_recv()
        compute_picked(m)

    def forward_up(*numbers):
        for piece in numbers:
            slab_copy(0, piece).wait_recv()
            slab_copy(2, piece).start()

    def forward_down(piece):
        slab_copy(1, piece).wait_recv()
        slab_copy(3, piece).start()
        if piece + AHEAD < pieces:
            slab_copy(1, piece + AHEAD).start()

    def cross(piece):
        slab_copy(3, piece).wait_recv()
        slab_copy(4, piece).start()

    send(0)
    forward_down(0)
    loads[1].wait()
    loads[2].wait()
    parts[...] = jnp.zeros_like(parts)
    compute_slab(0)
    forward_down(1)
    table_copy(1).wait_recv()
    table_copy(4).wait_recv()
    for k in (2, 3, 5):
        table_copy(k).start()
    forward_up(0, 1)
    forward_down(2)
    forward_up(2)
    cross(0)
    forward_up(3)
    forward_down(3)
    forward_up(4)
    cross(1)
    forward_up(5)
    forward_down(4)
    forward_up(6, 7)
    send(1)
    cross(2)
    compute_slab(1)
    forward_down(5)
    receive(0)
    cross(3)
    forward_down(6)
    cross(4)
    forward_down(7)
    send(2)
    compute_slab(2)
    cross(5)
    for k in (2, 3, 5):
        table_copy(k).wait_recv()
    rest = pl.ds(1, len(TABLE_TO) - 1)
    far_to_smem = pltpu.make_async_copy(tables.at[rest], far_smem.at[rest], load_sem.at[10])
    far_to_smem.start()
    cross(6)
    cross(7)
    far_to_smem.wait()

    all_of(2).wait_recv()
    send(6, 7, 4, 5, 3)
    compute_slab(3)
    compute_slab(4)
    all_of(4).wait_recv()
    send(9, 8)
    compute_slab(5)
    for m in (1, 2, 7, 6, 3, 9, 4, 5, 8):
        receive(m)

    others = pl.ds(1, 15)
    early = pl.ds(1, 15 - LATE)

    def wait_bytes(ref, semaphore):
        pltpu.make_async_copy(ref, ref, semaphore).wait()

    def put(lo, hi):
        for g in range(lo, hi):
            dep_out[g] = deps[my_smem[2, g]]

    put(0, 4)
    send_part()
    put(4, 16)
    total = parts[0]
    wait_bytes(from_tm.at[early, rows], tm_recv.at[0])
    for q in range(1, 16 - LATE):
        total = total + from_tm[q]
    row_sum[...] = total
    put(16, 20)

    def obs_copy(step):
        return pltpu.make_async_remote_copy(
            src_ref=row_sum.at[rows], dst_ref=from_obs.at[step, rows],
            send_sem=obs_send.at[0], recv_sem=obs_recv.at[0],
            device_id={"obs": lax.rem(obs + step, n_obs)}, device_id_type=MESH,
        )

    for step in range(1, n_obs):
        obs_copy(step).start()
    put(20, 32)

    for flow in range(len(FLOWS)):
        all_of(flow).wait_send()
    wait_bytes(tables, table_send.at[0])
    wait_bytes(outgoing, pick_send.at[0])
    wait_bytes(from_tm.at[early, rows], tm_send.at[0])

    wait_bytes(from_obs.at[others, rows], obs_recv.at[0])
    for step in range(1, n_obs):
        total = total + from_obs[step]
    wait_bytes(from_late.at[pl.ds(0, LATE), pl.ds(0, n_obs), rows], late_recv.at[0])
    for number in range(LATE):
        for step in range(n_obs):
            total = total + from_late[number, step]
    sums_out[...] = total
    wait_bytes(from_obs.at[others, rows], obs_send.at[0])
    wait_bytes(from_late.at[pl.ds(0, LATE), pl.ds(0, n_obs), rows], late_send.at[0])


def per_device(trajectory, weights, observed, window, block, counts, flags, inv_error):
    groups, slots, columns = weights.shape
    levels = observed.shape[2]
    blocks = trajectory.shape[1]
    bf16, f32, i32 = jnp.bfloat16, jnp.float32, jnp.int32
    dma = pltpu.SemaphoreType.DMA
    pieces = blocks // PIECE
    picks, tables = len(PICKS), len(TABLE_TO)
    any_space = pl.BlockSpec(memory_space=pl.ANY)
    vmem = pl.BlockSpec(memory_space=pltpu.VMEM)
    slab = pltpu.VMEM((blocks, columns, levels), bf16)
    arrays = (
        trajectory, weights, observed, window.reshape(1, groups), block.reshape(1, groups),
        counts.reshape(1, groups), flags, inv_error.reshape(1, levels),
    )
    departures, sums = pl.pallas_call(
        kernel,
        out_shape=(
            jax.ShapeDtypeStruct((groups, slots, levels), bf16),
            jax.ShapeDtypeStruct((8, levels), f32),
        ),
        in_specs=[any_space] * 8,
        out_specs=(vmem, vmem),
        scratch_shapes=[
            slab, slab, slab, slab, slab, slab,
            pltpu.VMEM((picks, GCAP, columns, levels), bf16),
            pltpu.VMEM((picks, GCAP, columns, levels), bf16),
            pltpu.VMEM((groups, slots, columns), bf16),
            pltpu.VMEM((groups, slots, levels), bf16),
            pltpu.VMEM((16 * GCAP, slots, levels), bf16),
            pltpu.VMEM((slots, groups), bf16),
            pltpu.VMEM((1, groups), i32),
            pltpu.VMEM((1, groups), i32),
            pltpu.VMEM((1, groups), i32),
            pltpu.VMEM((groups, slots), i32),
            pltpu.VMEM((1, levels), f32),
            pltpu.VMEM((8, 128), i32),
            pltpu.VMEM((tables, 8, 128), i32),
            pltpu.VMEM((16, 8, levels), f32),
            pltpu.VMEM((16, 8, levels), f32),
            pltpu.VMEM((8, levels), f32),
            pltpu.VMEM((16, 8, levels), f32),
            pltpu.VMEM((LATE, 16, 8, levels), f32),
            pltpu.SMEM((8, 128), i32),
            pltpu.SMEM((tables, 8, 128), i32),
            dma((11,)),
            dma((len(FLOWS),)), dma((3 * pieces,)), dma((2,)),
            dma((1,)), dma((picks,)),
            dma((1,)), dma((tables,)),
            dma((1,)), dma((1,)),
            dma((1,)), dma((1,)),
            dma((1,)), dma((1,)),
        ],
        compiler_params=pltpu.CompilerParams(
            collective_id=0, has_side_effects=True, vmem_limit_bytes=40 * 2**20
        ),
        name="exchange_and_check",
    )(*(pltpu.with_memory_space_constraint(array, pltpu.HBM) for array in arrays))
    plus_one = sums[2:3] + 1.0
    return departures, sums[0:1] / jnp.sqrt(plus_one), sums[1:2] / plus_one


def solution(mesh):
    both = ("tm", "obs")
    return jax.shard_map(
        per_device,
        mesh=mesh,
        in_specs=(
            P("tm", "obs", None, None),
            P(both, None, None),
            P(both, None, None),
            P(both, None),
            P(both),
            P(both),
            P(both, None),
            P(),
        ),
        out_specs=(P(both, None, None), P("tm", None), P("tm", None)),
        check_vma=False,
    )
```
